8 devices in a mesh: f: 2 (over z, y), h: 4 (over x, core).
Axes of the slice: x: 2, y: 2, z: 1, core: 2. Of those that a mesh axis runs over, the one named last changes fastest.
Arguments:
- x: bfloat16 [512, 4096], P(None, 'h')
- g1: float32 [4096], P('h')
- g2: float32 [4096], P('h')
- w_gate: bfloat16 [4096, 14336], P('h', 'f')
- w_up: bfloat16 [4096, 14336], P('h', 'f')
- w_down: bfloat16 [14336, 4096], P('f', 'h')
- o: bfloat16 [512, 4096], P(None, 'f')
- w_o: bfloat16 [4096, 4096], P('f', 'h')
- w_qkv: bfloat16 [4096, 6144], P('h', 'f')
Outputs:
- output 1: bfloat16 [512, 4096], P(None, 'h')
- output 2: bfloat16 [512, 6144], P(None, 'f')
All inputs are finite; a program needn't handle non-finite values.
Results may differ from the reference program's by a relative error of at most 0.00394098.
Values are sent between devices in bfloat16 or wider.
A program may use at most 1 GiB of HBM per device.

```python
import jax
import jax.numpy as jnp
from jax import lax

T = 512
D = 4096
FF = 14336
HEADS = 32
KV_HEADS = 8
HEAD = 128
HD = HEADS * HEAD
Q = (HEADS + 2 * KV_HEADS) * HEAD
EPS = 1e-6


def _w(key, shape):
    return (jax.random.normal(key, shape, jnp.float32) * shape[0] ** -0.5).astype(jnp.bfloat16)


def setup_inputs(seed: int = 0) -> dict:
    ks = jax.random.split(jax.random.PRNGKey(seed), 11)
    z = jax.random.normal(ks[0], (T, D), jnp.float32)
    row = jnp.exp(jax.random.uniform(ks[1], (T, 1), jnp.float32, -1.0, 1.0))
    tilt = jax.random.uniform(ks[2], (T, 1), jnp.float32, -1.0, 1.0)
    pos = jnp.arange(D, dtype=jnp.float32)[None, :] * (2.0 / D) - 1.0
    x = (z * row * jnp.exp(tilt * pos)).astype(jnp.bfloat16)
    o = (0.7 * jax.random.normal(ks[8], (T, HD), jnp.float32)).astype(jnp.bfloat16)
    return {
        'x': x,
        'g1': jax.random.uniform(ks[3], (D,), jnp.float32, 0.5, 1.5),
        'g2': jax.random.uniform(ks[4], (D,), jnp.float32, 0.5, 1.5),
        'w_gate': _w(ks[5], (D, FF)),
        'w_up': _w(ks[6], (D, FF)),
        'w_down': _w(ks[7], (FF, D)),
        'o': o,
        'w_o': _w(ks[9], (HD, D)),
        'w_qkv': _w(ks[10], (D, Q)),
    }


def _norm(x, g):
    xf = x.astype(jnp.float32)
    r = lax.rsqrt(jnp.mean(xf * xf, axis=-1, keepdims=True) + EPS)
    return (xf * r * g).astype(jnp.bfloat16)


def reference(x, g1, g2, w_gate, w_up, w_down, o, w_o, w_qkv):
    n = _norm(x, g1)
    gt = jnp.dot(n, w_gate, preferred_element_type=jnp.float32)
    up = jnp.dot(n, w_up, preferred_element_type=jnp.float32)
    a = (jax.nn.silu(gt) * up).astype(jnp.bfloat16)
    y = jnp.dot(a, w_down, preferred_element_type=jnp.float32) + jnp.dot(o, w_o, preferred_element_type=jnp.float32)
    x_next = (x.astype(jnp.float32) + y).astype(jnp.bfloat16)
    n1 = _norm(x_next, g2)
    qkv = jnp.dot(n1, w_qkv, preferred_element_type=jnp.float32).astype(jnp.bfloat16)
    return (x_next, qkv)
```

```python
import functools

import jax
import jax.numpy as jnp
from jax import lax
from jax.experimental import pallas as pl
from jax.experimental.pallas import tpu as pltpu
from jax.sharding import PartitionSpec as P

EPS = 1e-6
MESH = pl.DeviceIdType.MESH
F32 = jnp.float32
BF16 = jnp.bfloat16
NT = 256
NB = 3


def _dot(a, b):
    return jnp.dot(a, b, preferred_element_type=F32)


def _kernel(T, C, d,
            x_hbm, g1_hbm, g2_hbm, wg_hbm, wu_hbm, wd_hbm, o_hbm, wo_hbm, wq_hbm,
            xo_hbm, qo_hbm, wsib_hbm,
            xv, g1v, g2v, ov, wd, wo, wq, wbuf, nf, ss1, psnd, prcv, pkeep, abuf, ysnd, yrcv, xov, ss2, nf2,
            qsnd, qrcv, qkeep, qall,
            in_sem, ld_sem, ws_s, ws_r, wq_s, wq_r, n_s, n_r, ss1_s, ss1_r, p_s, p_r, a_s, a_r, y_s, y_r, ss2_s, ss2_r,
            n2_s, n2_r, q_s, q_r, qa_s, qa_r, out_sem):
    S = xv.shape[0]
    HL = xv.shape[1]
    FB = abuf.shape[3]
    QB = qall.shape[3]
    TP = FB // NT
    QT = QB // NT
    DT = HL // NT
    f = lax.axis_index('f')
    h = lax.axis_index('h')
    c = lax.rem(h, 2)
    xx = h // 2
    hx = (1 - xx) * 2 + c
    hs = xx * 2 + (1 - c)
    hd = (1 - xx) * 2 + (1 - c)
    XP, SIB, DIAG, YP = (f, hx), (f, hs), (f, hd), (1 - f, h)

    def rcopy(src, dst, s, r, dev):
        return pltpu.make_async_remote_copy(src_ref=src, dst_ref=dst, send_sem=s, recv_sem=r, device_id=dev,
                                            device_id_type=MESH)

    def lcopy(src, dst, s):
        return pltpu.make_async_copy(src, dst, s)

    def mo(v, m):
        return pl.multiple_of(v, m)

    first = [lcopy(x_hbm, xv, in_sem.at[0]), lcopy(g1_hbm, g1v, in_sem.at[1]), lcopy(g2_hbm, g2v, in_sem.at[2])]
    for cp in first:
        cp.start()

    bar = pltpu.get_barrier_semaphore()
    for dev in (XP, SIB, DIAG, YP):
        pl.semaphore_signal(bar, inc=1, device_id=dev, device_id_type=MESH)
    pl.semaphore_wait(bar, 4)

    def wcopy(t, m):
        blk = jnp.where(t < TP, hd, hs)
        col = mo(blk * FB + lax.rem(t, TP) * NT, NT)
        src = (wg_hbm, wu_hbm)[m].at[:, pl.ds(col, NT)]
        return rcopy(src, wsib_hbm.at[t, m], ws_s.at[t, m], ws_r.at[t, m], SIB)

    def wqcopy(b, t):
        blk = (hd, hs)[b]
        col = mo(blk * QB + t * NT, NT)
        return rcopy(wq_hbm.at[:, pl.ds(col, NT)], wq.at[b, t, pl.ds(HL, HL)], wq_s.at[b, t], wq_r.at[b, t], SIB)

    for m in range(2):
        wcopy(jnp.int32(0), m).start()
    for cp in first:
        cp.wait()

    for j in range(S // 128):
        xf = xv[pl.ds(j * 128, 128), :].astype(F32)
        s = jnp.sum(xf * xf, axis=1, keepdims=True)
        ss1[h, :, pl.ds(j * 128, 128)] = jnp.broadcast_to(s, (128, 128)).T[0:8]

    def ss1copy(k):
        dev = (XP, SIB, DIAG)[k]
        return rcopy(ss1.at[h], ss1.at[h], ss1_s.at[k], ss1_r.at[k], dev)

    for k in range(3):
        ss1copy(k).start()
    for k in range(3):
        ss1copy(k).wait()
    r1 = lax.rsqrt((ss1[0] + ss1[1] + ss1[2] + ss1[3]) / d + EPS)
    for j in range(S // 128):
        rr = jnp.broadcast_to(r1[0:1, j * 128:(j + 1) * 128], (128, 128)).T
        for l in range(HL // 128):
            xf = xv[pl.ds(j * 128, 128), pl.ds(l * 128, 128)].astype(F32)
            nf[pl.ds(j * 128, 128), pl.ds(l * 128, 128)] = (xf * rr * g1v[:, pl.ds(l * 128, 128)]).astype(BF16)
    ncp = rcopy(nf.at[:, pl.ds(0, HL)], nf.at[:, pl.ds(HL, HL)], n_s, n_r, SIB)
    ncp.start()

    @pl.loop(1, 2 * TP)
    def _(t):
        for m in range(2):
            wcopy(t, m).start()

    for b in range(2):
        for t in range(QT):
            wqcopy(b, t).start()

    def loads(g):
        t = lax.rem(g, 2 * TP)
        bs = lax.rem(g, NB)
        blk = jnp.where(t < TP, hx, h)
        col = mo(blk * FB + lax.rem(t, TP) * NT, NT)
        return (lcopy(wg_hbm.at[:, pl.ds(col, NT)], wbuf.at[bs, 0, pl.ds(0, HL)], ld_sem.at[bs, 0]),
                lcopy(wu_hbm.at[:, pl.ds(col, NT)], wbuf.at[bs, 1, pl.ds(0, HL)], ld_sem.at[bs, 1]),
                lcopy(wsib_hbm.at[t, 0], wbuf.at[bs, 0, pl.ds(HL, HL)], ld_sem.at[bs, 2]),
                lcopy(wsib_hbm.at[t, 1], wbuf.at[bs, 1, pl.ds(HL, HL)], ld_sem.at[bs, 3]))

    def start_load(g):
        cps = loads(g)
        cps[0].start()
        cps[1].start()

        @pl.when(g < 2 * TP)
        def _():
            for m in range(2):
                wcopy(g, m).wait_recv()

        cps[2].start()
        cps[3].start()

    def pcopy(j, t):
        s2 = lax.rem(j, 2)
        s3 = lax.rem(j, 3)
        return rcopy(psnd.at[s2, t], prcv.at[s3, t], p_s.at[s2, t], p_r.at[s3, t], XP)

    def gu(j, t):
        g = j * (2 * TP) + t
        bs = lax.rem(g, NB)
        for cp in loads(g):
            cp.wait()

        @pl.when(g + NB - 1 < C * 2 * TP)
        def _():
            start_load(g + NB - 1)

        nn = nf[pl.ds(mo(j * T, T), T), :]
        return _dot(nn, wbuf[bs, 0]), _dot(nn, wbuf[bs, 1])

    def s12(j):
        s2 = lax.rem(j, 2)

        @pl.loop(0, TP)
        def _(t):
            @pl.when(j >= 2)
            def _():
                pcopy(j - 2, t).wait_send()

            gg, uu = gu(j, t)
            psnd[s2, t, :, 0:NT] = gg
            psnd[s2, t, :, NT:2 * NT] = uu
            pcopy(j, t).start()

        @pl.loop(0, TP)
        def _(t):
            gg, uu = gu(j, t + TP)
            pkeep[s2, t, :, 0:NT] = gg
            pkeep[s2, t, :, NT:2 * NT] = uu

    def acopy(i, k):
        s2 = lax.rem(i, 2)
        if k == 0:
            return rcopy(abuf.at[s2, h], abuf.at[s2, h], a_s.at[s2, 0], a_r.at[s2, 0], XP)
        if k == 1:
            return rcopy(abuf.at[s2, h], abuf.at[s2, h], a_s.at[s2, 1], a_r.at[s2, 1], SIB)
        return rcopy(abuf.at[s2, hx], abuf.at[s2, hx], a_s.at[s2, 2], a_r.at[s2, 2], SIB)

    def s3(i):
        s2 = lax.rem(i, 2)
        sl3 = lax.rem(i, 3)

        @pl.loop(0, TP)
        def _(t):
            pcopy(i, t).wait_recv()
            gg = pkeep[s2, t, :, 0:NT] + prcv[sl3, t, :, 0:NT]
            uu = pkeep[s2, t, :, NT:2 * NT] + prcv[sl3, t, :, NT:2 * NT]
            abuf[s2, h, :, pl.ds(mo(t * NT, NT), NT)] = (gg * jax.nn.sigmoid(gg) * uu).astype(BF16)

        acopy(i, 0).start()
        acopy(i, 1).start()

    def ycopy(i):
        s2 = lax.rem(i, 2)
        return rcopy(ysnd.at[s2], yrcv.at[i], y_s.at[s2], y_r.at[i], YP)

    def s4(i):
        s2 = lax.rem(i, 2)
        acopy(i, 0).wait_recv()
        acopy(i, 2).start()
        acopy(i, 1).wait_recv()
        acopy(i, 2).wait_recv()

        @pl.loop(0, DT)
        def _(n):
            acc = _dot(ov[pl.ds(mo(i * T, T), T), :], wo[n])
            for b in range(4):
                acc += _dot(abuf[s2, b], wd[n, b * FB:(b + 1) * FB])
            ysnd[s2, :, pl.ds(mo(n * NT, NT), NT)] = acc

        ycopy(i).start()

    def ss2copy(i, k):
        dev = (XP, SIB, DIAG)[k]
        return rcopy(ss2.at[i, h], ss2.at[i, h], ss2_s.at[i, k], ss2_r.at[i, k], dev)

    def xocopy(i):
        rows = pl.ds(mo(i * T, T), T)
        return lcopy(xov.at[rows], xo_hbm.at[rows], out_sem.at[i, 4])

    def s5(i):
        s2 = lax.rem(i, 2)
        for k in range(3):
            acopy(i, k).wait_send()
        ycopy(i).wait()
        rows = pl.ds(mo(i * T, T), T)
        xn = (xv[rows, :].astype(F32) + (ysnd[s2] + yrcv[i])).astype(BF16)
        xov[rows, :] = xn
        xf = xn.astype(F32)
        s = jnp.broadcast_to(jnp.sum(xf * xf, axis=1, keepdims=True), (T, 128))
        if T < 128:
            s = jnp.concatenate([s] * (128 // T), axis=0)
        ss2[i, h] = s.T[0:8]
        for k in range(3):
            ss2copy(i, k).start()
        xocopy(i).start()

    def n2copy(i):
        rows = pl.ds(mo(i * T, T), T)
        return rcopy(nf2.at[rows, pl.ds(0, HL)], nf2.at[rows, pl.ds(HL, HL)], n2_s.at[i], n2_r.at[i], SIB)

    def s6(i):
        rows = pl.ds(mo(i * T, T), T)
        for k in range(3):
            ss2copy(i, k).wait_recv()
        r = lax.rsqrt((ss2[i, 0] + ss2[i, 1] + ss2[i, 2] + ss2[i, 3]) / d + EPS)
        rr = jnp.broadcast_to(r[0:1], (128, 128)).T[0:T]
        for l in range(HL // 128):
            xf = xov[rows, pl.ds(l * 128, 128)].astype(F32)
            nf2[rows, pl.ds(l * 128, 128)] = (xf * rr * g2v[:, pl.ds(l * 128, 128)]).astype(BF16)
        n2copy(i).start()

    def qcopy(i):
        return rcopy(qsnd.at[i], qrcv.at[i], q_s.at[i], q_r.at[i], XP)

    def s7(i):
        n2copy(i).wait_recv()
        nn = nf2[pl.ds(mo(i * T, T), T), :]
        for t in range(QT):
            qsnd[i, :, t * NT:(t + 1) * NT] = _dot(nn, wq[0, t])
        qcopy(i).start()
        for t in range(QT):
            qkeep[i, :, t * NT:(t + 1) * NT] = _dot(nn, wq[1, t])

    def qacopy(i, k):
        b = (h, h, hx)[k]
        dev = (XP, SIB, SIB)[k]
        return rcopy(qall.at[i, b], qall.at[i, b], qa_s.at[i, k], qa_r.at[i, k], dev)

    def s8(i):
        qcopy(i).wait_recv()
        qall[i, h] = (qkeep[i] + qrcv[i]).astype(BF16)
        qacopy(i, 0).start()
        qacopy(i, 1).start()

    def qocopy(i, b):
        return lcopy(qall.at[i, b], qo_hbm.at[pl.ds(mo(i * T, T), T), pl.ds(b * QB, QB)], out_sem.at[i, b])

    def s9(i):
        qacopy(i, 0).wait_recv()
        qacopy(i, 2).start()
        qacopy(i, 1).wait_recv()
        qacopy(i, 2).wait_recv()
        for b in range(4):
            qocopy(i, b).start()

    ncp.wait_recv()
    for g in range(NB - 1):
        start_load(jnp.int32(g))

    res = [lcopy(o_hbm, ov, in_sem.at[3])]
    for n in range(DT):
        res.append(lcopy(wd_hbm.at[:, pl.ds(n * NT, NT)], wd.at[n], in_sem.at[4 + n]))
        res.append(lcopy(wo_hbm.at[:, pl.ds(n * NT, NT)], wo.at[n], in_sem.at[4 + DT + n]))
    for b in range(2):
        blk = (hx, h)[b]
        for t in range(QT):
            res.append(lcopy(wq_hbm.at[:, pl.ds(mo(blk * QB + t * NT, NT), NT)], wq.at[b, t, pl.ds(0, HL)],
                             in_sem.at[4 + 2 * DT + b * QT + t]))

    @pl.loop(0, 2)
    def _(j):
        s12(j)

        @pl.when(j == 0)
        def _():
            for cp in res:
                cp.start()

    for cp in res:
        cp.wait()
    for b in range(2):
        for t in range(QT):
            wqcopy(b, t).wait()

    def stage(fn, i):
        @pl.when((i >= 0) & (i < C))
        def _():
            fn(i)

    @pl.loop(0, C + 3)
    def _(i):
        stage(s3, i)
        stage(s12, i + 2)
        stage(s5, i - 1)
        stage(s4, i)
        stage(s6, i - 1)
        stage(s8, i - 2)
        stage(s7, i - 1)
        stage(s9, i - 3)

    ncp.wait_send()

    @pl.loop(0, 2 * TP)
    def _(t):
        for m in range(2):
            wcopy(t, m).wait_send()

    @pl.loop(0, TP)
    def _(t):
        pcopy(C - 2, t).wait_send()
        pcopy(C - 1, t).wait_send()

    @pl.loop(0, C)
    def _(i):
        for k in range(3):
            ss2copy(i, k).wait_send()
            qacopy(i, k).wait_send()
        n2copy(i).wait_send()
        qcopy(i).wait_send()
        xocopy(i).wait()
        for b in range(4):
            qocopy(i, b).wait()


def solution(mesh):
    nh = mesh.shape['h']

    def body(x, g1, g2, w_gate, w_up, w_down, o, w_o, w_qkv):
        S, HL = x.shape
        FL = w_gate.shape[1]
        FB = FL // nh
        QL = w_qkv.shape[1]
        QB = QL // nh
        OL = o.shape[1]
        T = 64
        C = S // T
        TP, QT, DT = FB // NT, QB // NT, HL // NT
        d = HL * nh
        any_ = pl.BlockSpec(memory_space=pl.ANY)
        dma = pltpu.SemaphoreType.DMA
        V = pltpu.VMEM
        scratch = [
            V((S, HL), BF16), V((1, HL), F32), V((1, HL), F32), V((S, OL), BF16),
            V((DT, FL, NT), BF16), V((DT, OL, NT), BF16), V((2, QT, 2 * HL, NT), BF16),
            V((NB, 2, 2 * HL, NT), BF16), V((S, 2 * HL), BF16), V((nh, 8, S), F32),
            V((2, TP, T, 2 * NT), F32), V((3, TP, T, 2 * NT), F32), V((2, TP, T, 2 * NT), F32),
            V((2, nh, T, FB), BF16), V((2, T, HL), F32), V((C, T, HL), F32), V((S, HL), BF16),
            V((C, nh, 8, 128), F32), V((S, 2 * HL), BF16),
            V((C, T, QB), F32), V((C, T, QB), F32), V((C, T, QB), F32), V((C, nh, T, QB), BF16),
            dma((4 + 2 * DT + 2 * QT,)), dma((NB, 4)), dma((2 * TP, 2)), dma((2 * TP, 2)), dma((2, QT)), dma((2, QT)),
            dma, dma, dma((3,)), dma((3,)), dma((2, TP)), dma((3, TP)), dma((2, 3)), dma((2, 3)), dma((2,)), dma((C,)),
            dma((C, 3)), dma((C, 3)), dma((C,)), dma((C,)), dma((C,)), dma((C,)), dma((C, 3)), dma((C, 3)),
            dma((C, 5)),
        ]
        xo, qo, _ = pl.pallas_call(
            functools.partial(_kernel, T, C, float(d)),
            out_shape=(jax.ShapeDtypeStruct((S, HL), BF16), jax.ShapeDtypeStruct((S, QL), BF16),
                       jax.ShapeDtypeStruct((2 * TP, 2, HL, NT), BF16)),
            in_specs=[any_] * 9,
            out_specs=(any_, any_, any_),
            scratch_shapes=scratch,
            compiler_params=pltpu.CompilerParams(collective_id=0, has_side_effects=True, vmem_limit_bytes=67043328),
            name='block',
        )(x, g1.reshape(1, HL), g2.reshape(1, HL), w_gate, w_up, w_down, o, w_o, w_qkv)
        return xo, qo

    in_specs = (P(None, 'h'), P('h'), P('h'), P('h', 'f'), P('h', 'f'), P('f', 'h'),
                P(None, 'f'), P('f', 'h'), P('h', 'f'))
    return jax.shard_map(body, mesh=mesh, in_specs=in_specs,
                         out_specs=(P(None, 'h'), P(None, 'f')), check_vma=False)
```

```python
import functools

import jax
import jax.numpy as jnp
from jax import lax
from jax.experimental import pallas as pl
from jax.experimental.pallas import tpu as pltpu
from jax.sharding import PartitionSpec as P

EPS = 1e-6
MESH = pl.DeviceIdType.MESH
F32 = jnp.float32
BF16 = jnp.bfloat16
NT = 256
NB = 3


def _dot(a, b):
    return jnp.dot(a, b, preferred_element_type=F32)


def _kernel(T, C, d,
            x_hbm, g1_hbm, g2_hbm, wg_hbm, wu_hbm, wd_hbm, o_hbm, wo_hbm, wq_hbm,
            xov, qall, wsib_hbm,
            xv, g1v, g2v, ov, wd, wo, wq, wbuf, nf, ss1, psnd, prcv, pkeep, abuf, ysnd, yrcv, ss2, nf2,
            qsnd, qrcv, qkeep,
            in_sem, ld_sem, ws_s, ws_r, wq_s, wq_r, n_s, n_r, ss1_s, ss1_r, p_s, p_r, a_s, a_r, y_s, y_r, ss2_s, ss2_r,
            n2_s, n2_r, q_s, q_r, qa_s, qa_r):
    S = xv.shape[0]
    HL = xv.shape[1]
    FB = abuf.shape[3]
    QB = qsnd.shape[2]
    TP = FB // NT
    QT = QB // NT
    DT = HL // NT
    f = lax.axis_index('f')
    h = lax.axis_index('h')
    c = lax.rem(h, 2)
    xx = h // 2
    hx = (1 - xx) * 2 + c
    hs = xx * 2 + (1 - c)
    hd = (1 - xx) * 2 + (1 - c)
    XP, SIB, DIAG, YP = (f, hx), (f, hs), (f, hd), (1 - f, h)

    def rcopy(src, dst, s, r, dev):
        return pltpu.make_async_remote_copy(src_ref=src, dst_ref=dst, send_sem=s, recv_sem=r, device_id=dev,
                                            device_id_type=MESH)

    def lcopy(src, dst, s):
        return pltpu.make_async_copy(src, dst, s)

    def lwait(ref, sem):
        lcopy(ref, ref, sem).wait()

    def rwait(ref, sem):
        rcopy(ref, ref, sem, sem, XP).wait_recv()

    def mo(v, m):
        return pl.multiple_of(v, m)

    first = [lcopy(x_hbm, xv, in_sem.at[0]), lcopy(g1_hbm, g1v.at[:, pl.ds(0, HL)], in_sem.at[1]),
             lcopy(g2_hbm, g2v, in_sem.at[2])]
    for cp in first:
        cp.start()

    bar = pltpu.get_barrier_semaphore()
    for dev in (XP, SIB, DIAG, YP):
        pl.semaphore_signal(bar, inc=1, device_id=dev, device_id_type=MESH)

    NL = 3 * TP + (C - 2) * 2 * TP

    def tile_of(g):
        return jnp.where(g < TP, g, lax.rem(g + TP, 2 * TP))

    def own(g):
        t = tile_of(g)
        bs = lax.rem(g, NB)
        blk = jnp.where(t < TP, hx, h)
        col = mo(blk * FB + lax.rem(t, TP) * NT, NT)
        return (lcopy(wg_hbm.at[:, pl.ds(col, NT)], wbuf.at[bs, 0, pl.ds(0, HL)], ld_sem.at[bs]),
                lcopy(wu_hbm.at[:, pl.ds(col, NT)], wbuf.at[bs, 1, pl.ds(0, HL)], ld_sem.at[bs]))

    def sib(g):
        t = tile_of(g)
        bs = lax.rem(g, NB)
        return (lcopy(wsib_hbm.at[t, 0], wbuf.at[bs, 0, pl.ds(HL, HL)], ld_sem.at[bs]),
                lcopy(wsib_hbm.at[t, 1], wbuf.at[bs, 1, pl.ds(HL, HL)], ld_sem.at[bs]))

    def wcopy(t, m):
        blk = jnp.where(t < TP, hd, hs)
        col = mo(blk * FB + lax.rem(t, TP) * NT, NT)
        src = (wg_hbm, wu_hbm)[m].at[:, pl.ds(col, NT)]
        return rcopy(src, wsib_hbm.at[t, m], ws_s, ws_r.at[t], SIB)

    def wqcopy(b, t):
        blk = (hd, hs)[b]
        col = mo(blk * QB + t * NT, NT)
        return rcopy(wq_hbm.at[:, pl.ds(col, NT)], wq.at[b, t, pl.ds(HL, HL)], wq_s, wq_r, SIB)

    def start_sib(g):
        @pl.when((g < TP) | ((g >= 2 * TP) & (g < 3 * TP)))
        def _():
            t = tile_of(g)
            rwait(wsib_hbm.at[t], ws_r.at[t])

        for cp in sib(g):
            cp.start()

    def start_own(g):
        for cp in own(g):
            cp.start()

    def wait_tile(g):
        bs = lax.rem(g, NB)
        lwait(wbuf.at[bs], ld_sem.at[bs])

    for g in range(2):
        start_own(jnp.int32(g))
    for cp in first:
        cp.wait()

    R0 = 128
    for j in range(S // 128):
        xf = xv[pl.ds(j * 128, 128), :].astype(F32)
        s = jnp.sum(xf * xf, axis=1, keepdims=True)
        ss1[j, h] = jnp.broadcast_to(s, (128, 128)).T[0:1]

    def ss1copy(j, k):
        dev = (XP, SIB, DIAG)[k]
        return rcopy(ss1.at[j, h], ss1.at[j, h], ss1_s, ss1_r.at[min(j, 1)], dev)

    def xcopy(k):
        rows = (pl.ds(0, R0), pl.ds(R0, S - R0))[k]
        return rcopy(xv.at[rows], nf2.at[rows, pl.ds(HL, HL)], n_s.at[k], n_r.at[k], SIB)

    gcp = rcopy(g1v.at[:, pl.ds(0, HL)], g1v.at[:, pl.ds(HL, HL)], n_s.at[2], n_r.at[2], SIB)

    pl.semaphore_wait(bar, 4)
    for k in (0, 2, 1):
        ss1copy(0, k).start()
    xcopy(0).start()
    gcp.start()
    for m in range(2):
        wcopy(jnp.int32(0), m).start()
    for j in range(1, S // 128):
        for k in range(3):
            ss1copy(j, k).start()
    xcopy(1).start()

    @pl.loop(1, 2 * TP)
    def _(t):
        for m in range(2):
            wcopy(t, m).start()

    for b in range(2):
        for t in range(QT):
            wqcopy(b, t).start()


    def norm1(j):
        if j == 0:
            rwait(ss1.at[0, pl.ds(0, 3)], ss1_r.at[0])
        elif j == 1:
            rwait(ss1.at[pl.ds(1, S // 128 - 1), pl.ds(0, 3)], ss1_r.at[1])
        r1 = lax.rsqrt((ss1[j, 0] + ss1[j, 1] + ss1[j, 2] + ss1[j, 3]) / d + EPS)
        rr = jnp.broadcast_to(r1, (128, 128)).T
        rows = pl.ds(j * 128, 128)
        for half in range(2):
            for l in range(HL // 128):
                cols = pl.ds(half * HL + l * 128, 128)
                xb = xv[rows, pl.ds(l * 128, 128)] if half == 0 else nf2[rows, cols]
                nf[rows, cols] = (xb.astype(F32) * rr * g1v[:, cols]).astype(BF16)

    rwait(wsib_hbm.at[0], ws_r.at[0])
    for cp in sib(jnp.int32(0)):
        cp.start()
    gcp.wait_recv()
    xcopy(0).wait_recv()
    norm1(0)

    def pcopy(j, t):
        s2 = lax.rem(j, 2)
        s3 = lax.rem(j, 3)
        return rcopy(psnd.at[s2, t], prcv.at[s3, t], p_s.at[s2], p_r.at[s3], XP)

    def gu(g, row, n):
        bs = lax.rem(g, NB)
        nn = nf[pl.ds(row, n), :]
        return _dot(nn, wbuf[bs, 0]), _dot(nn, wbuf[bs, 1])

    def prefetch(g):
        @pl.when(g < NL)
        def _():
            start_own(g)
            start_sib(g)

    def put_send(j, t, gg, uu):
        s2 = lax.rem(j, 2)
        psnd[s2, t, :, 0:NT] = gg
        psnd[s2, t, :, NT:2 * NT] = uu
        pcopy(j, t).start()

    def s12(j):
        s2 = lax.rem(j, 2)
        g0 = 3 * TP + (j - 2) * (2 * TP)
        rwait(psnd.at[s2], p_s.at[s2])
        row = mo(j * T, T)

        @pl.loop(0, TP)
        def _(t):
            wait_tile(g0 + t)
            prefetch(g0 + t + NB - 1)
            gg, uu = gu(g0 + t, row, T)
            put_send(j, t, gg, uu)

        @pl.loop(0, TP)
        def _(t):
            wait_tile(g0 + t + TP)
            prefetch(g0 + t + TP + NB - 1)
            gg, uu = gu(g0 + t + TP, row, T)
            pkeep[s2, t, :, 0:NT] = gg
            pkeep[s2, t, :, NT:2 * NT] = uu

    def acopy(i, k):
        sl = lax.rem(i, 3)
        b = (h, h, hx)[k]
        return rcopy(abuf.at[sl, b], abuf.at[sl, b], a_s.at[sl, k], a_r.at[sl, k], (XP, SIB, SIB)[k])

    def s3(i):
        s2 = lax.rem(i, 2)
        sl = lax.rem(i, 3)

        rwait(prcv.at[sl], p_r.at[sl])

        @pl.loop(0, TP)
        def _(t):
            gg = pkeep[s2, t, :, 0:NT] + prcv[sl, t, :, 0:NT]
            uu = pkeep[s2, t, :, NT:2 * NT] + prcv[sl, t, :, NT:2 * NT]
            abuf[sl, h, :, pl.ds(mo(t * NT, NT), NT)] = (gg * jax.nn.sigmoid(gg) * uu).astype(BF16)

        acopy(i, 0).start()
        acopy(i, 1).start()

    def ycopy(i, n):
        s2 = lax.rem(i, 2)
        cols = pl.ds(mo(n * NT, NT), NT)
        sl = lax.rem(i, 3)
        return rcopy(ysnd.at[s2, :, cols], yrcv.at[sl, :, cols], y_s.at[s2], y_r.at[sl], YP)

    def down(sl, b, n):
        return _dot(abuf[sl, b], wd[n, pl.ds(mo(b * FB, FB), FB)])

    def s4a(i):
        s2 = lax.rem(i, 2)
        sl = lax.rem(i, 3)
        acopy(i, 1).wait_recv()

        @pl.loop(0, DT)
        def _(n):
            acc = _dot(ov[pl.ds(mo(i * T, T), T), :], wo[n])
            acc += down(sl, h, n)
            acc += down(sl, hs, n)
            ysnd[s2, :, pl.ds(mo(n * NT, NT), NT)] = acc

    def s4b(i):
        s2 = lax.rem(i, 2)
        sl = lax.rem(i, 3)
        acopy(i, 0).wait_recv()
        acopy(i, 2).start()
        acopy(i, 2).wait_recv()

        @pl.loop(0, DT)
        def _(n):
            ysnd[s2, :, pl.ds(mo(n * NT, NT), NT)] += down(sl, hx, n) + down(sl, hd, n)
            ycopy(i, n).start()

    def ss2copy(i, k):
        dev = (XP, SIB, DIAG)[k]
        return rcopy(ss2.at[i, h], ss2.at[i, h], ss2_s, ss2_r.at[i], dev)

    def s5(i):
        s2 = lax.rem(i, 2)
        for k in range(3):
            acopy(i, k).wait_send()
        sl = lax.rem(i, 3)
        rwait(ysnd.at[s2], y_s.at[s2])
        rwait(yrcv.at[sl], y_r.at[sl])
        rows = pl.ds(mo(i * T, T), T)
        xn = (xv[rows, :].astype(F32) + (ysnd[s2] + yrcv[sl])).astype(BF16)
        xov[rows, :] = xn
        xf = xn.astype(F32)
        s = jnp.broadcast_to(jnp.sum(xf * xf, axis=1, keepdims=True), (T, 128))
        if T < 128:
            s = jnp.concatenate([s] * (128 // T), axis=0)
        ss2[i, h] = s.T[0:1]
        for k in range(3):
            ss2copy(i, k).start()

    def n2copy(i):
        rows = pl.ds(mo(i * T, T), T)
        return rcopy(nf2.at[rows, pl.ds(0, HL)], nf2.at[rows, pl.ds(HL, HL)], n2_s, n2_r.at[i], SIB)

    def s6(i):
        rows = pl.ds(mo(i * T, T), T)
        rwait(ss2.at[i, pl.ds(0, 3)], ss2_r.at[i])
        r = lax.rsqrt((ss2[i, 0] + ss2[i, 1] + ss2[i, 2] + ss2[i, 3]) / d + EPS)
        rr = jnp.broadcast_to(r, (128, 128)).T[0:T]
        for l in range(HL // 128):
            xf = xov[rows, pl.ds(l * 128, 128)].astype(F32)
            nf2[rows, pl.ds(l * 128, 128)] = (xf * rr * g2v[:, pl.ds(l * 128, 128)]).astype(BF16)
        n2copy(i).start()

    def qcopy(i):
        return rcopy(qsnd.at[i], qrcv.at[i], q_s, q_r.at[i], XP)

    def s7(i):
        n2copy(i).wait_recv()
        nn = nf2[pl.ds(mo(i * T, T), T), :]
        for t in range(QT):
            qsnd[i, :, t * NT:(t + 1) * NT] = _dot(nn, wq[0, t])
        qcopy(i).start()
        for t in range(QT):
            qkeep[i, :, t * NT:(t + 1) * NT] = _dot(nn, wq[1, t])

    def qacopy(i, k):
        b = (h, h, hx)[k]
        dev = (XP, SIB, SIB)[k]
        blk = qall.at[pl.ds(mo(i * T, T), T), pl.ds(mo(b * QB, NT), QB)]
        return rcopy(blk, blk, qa_s, qa_r.at[i if k == 0 else C], dev)

    def s8(i):
        qcopy(i).wait_recv()
        for t in range(QT):
            cols = pl.ds(t * NT, NT)
            qall[pl.ds(mo(i * T, T), T), pl.ds(mo(h * QB + t * NT, NT), NT)] = (qkeep[i, :, cols] + qrcv[i, :, cols]).astype(BF16)
        qacopy(i, 0).start()
        qacopy(i, 1).start()

    def s9a(i):
        qacopy(i, 0).wait_recv()
        qacopy(i, 2).start()

    @pl.loop(0, TP)
    def _(t):
        wait_tile(t)
        gg, uu = gu(t, 0, T)
        put_send(jnp.int32(0), t, gg, uu)
        start_own(t + 2)
        start_sib(t + 1)

    start_sib(jnp.int32(TP + 1))

    @pl.loop(0, TP)
    def _(t):
        wait_tile(TP + t)
        prefetch(TP + t + NB - 1)
        gg, uu = gu(TP + t, T, T)
        put_send(jnp.int32(1), t, gg, uu)

    xcopy(1).wait_recv()
    for j in range(1, S // 128):
        norm1(j)

    res = [[] for _ in range(4)]
    for n in range(DT):
        res[n % 4].append(lcopy(wd_hbm.at[:, pl.ds(n * NT, NT)], wd.at[n], in_sem.at[4]))
        res[n % 4].append(lcopy(wo_hbm.at[:, pl.ds(n * NT, NT)], wo.at[n], in_sem.at[5]))
    res[0].append(lcopy(o_hbm, ov, in_sem.at[3]))
    for b in range(2):
        blk = (hx, h)[b]
        for t in range(QT):
            res[3].append(lcopy(wq_hbm.at[:, pl.ds(mo(blk * QB + t * NT, NT), NT)], wq.at[b, t, pl.ds(0, HL)],
                                in_sem.at[6]))

    @pl.loop(0, TP)
    def _(t):
        wait_tile(2 * TP + t)
        prefetch(2 * TP + t + NB - 1)
        for k in range(4):
            @pl.when(t == k)
            def _(k=k):
                for cp in res[k]:
                    cp.start()

        gg, uu = gu(2 * TP + t, 0, 2 * T)
        for j in range(2):
            pkeep[j, t, :, 0:NT] = gg[j * T:(j + 1) * T]
            pkeep[j, t, :, NT:2 * NT] = uu[j * T:(j + 1) * T]

    def stage(fn, i, lo=0):
        @pl.when((i >= lo) & (i < C))
        def _():
            fn(i)

    def loaded():
        lwait(ov, in_sem.at[3])
        lwait(wd, in_sem.at[4])
        lwait(wo, in_sem.at[5])
        lwait(wq.at[:, :, pl.ds(0, HL)], in_sem.at[6])
        rwait(wq.at[:, :, pl.ds(HL, HL)], wq_s)
        rwait(wq.at[:, :, pl.ds(HL, HL)], wq_r)

    @pl.loop(0, C - 2)
    def _(i):
        s3(i)
        s12(i + 2)

        @pl.when(i == 0)
        def _():
            loaded()

        stage(s5, i - 1)
        s4a(i)
        s4b(i)
        stage(s6, i - 2)

    e = C - 1
    done = {s7: 0, s8: 0, s9a: 0}

    def run(*steps):
        for fn, i in steps:
            fn(jnp.int32(i))

    def nxt(*fns):
        for fn in fns:
            if done[fn] < C:
                fn(jnp.int32(done[fn]))
                done[fn] += 1

    run((s3, e - 1), (s4a, e - 1), (s5, e - 2), (s6, e - 3), (s3, e))
    nxt(s7)
    run((s4b, e - 1))
    nxt(s7)
    run((s4a, e), (s6, e - 2), (s4b, e))
    nxt(s7, s8)
    run((s5, e - 1))
    nxt(s7, s8)
    run((s5, e), (s6, e - 1))
    nxt(s7, s8)
    run((s6, e))
    nxt(s7, s8, s9a, s7, s8, s9a, s7, s8, s9a)
    gcp.wait_send()
    rwait(ss1.at[:, pl.ds(0, 3)], ss1_s)
    for k in range(2):
        xcopy(k).wait_send()

    rwait(wsib_hbm, ws_s)

    for k in range(2):
        rwait(psnd.at[k], p_s.at[k])

    while done[s8] < C:
        nxt(s8, s9a)

    rwait(ss2.at[:, pl.ds(0, 3)], ss2_s)
    rwait(nf2.at[:, pl.ds(0, HL)], n2_s)
    rwait(qsnd, q_s)

    while done[s9a] < C:
        nxt(s9a)
    rwait(qall.at[:, pl.ds(0, 2 * QB)], qa_r.at[C])
    rwait(qall.at[:, pl.ds(0, 3 * QB)], qa_s)


def solution(mesh):
    nh = mesh.shape['h']

    def body(x, g1, g2, w_gate, w_up, w_down, o, w_o, w_qkv):
        S, HL = x.shape
        FL = w_gate.shape[1]
        FB = FL // nh
        QL = w_qkv.shape[1]
        QB = QL // nh
        OL = o.shape[1]
        T = 64
        C = S // T
        TP, QT, DT = FB // NT, QB // NT, HL // NT
        d = HL * nh
        any_ = pl.BlockSpec(memory_space=pl.ANY)
        vm = pl.BlockSpec(memory_space=pltpu.VMEM)
        dma = pltpu.SemaphoreType.DMA
        V = pltpu.VMEM
        scratch = [
            V((S, HL), BF16), V((1, 2 * HL), F32), V((1, HL), F32), V((S, OL), BF16),
            V((DT, FL, NT), BF16), V((DT, OL, NT), BF16), V((2, QT, 2 * HL, NT), BF16),
            V((NB, 2, 2 * HL, NT), BF16), V((S, 2 * HL), BF16), V((S // 128, nh, 1, 128), F32),
            V((2, TP, T, 2 * NT), F32), V((3, TP, T, 2 * NT), F32), V((2, TP, T, 2 * NT), F32),
            V((3, nh, T, FB), BF16), V((2, T, HL), F32), V((3, T, HL), F32),
            V((C, nh, 1, 128), F32), V((S, 2 * HL), BF16),
            V((C, T, QB), F32), V((C, T, QB), F32), V((C, T, QB), F32),
            dma((7,)), dma((NB,)), dma, dma((2 * TP,)), dma, dma,
            dma((3,)), dma((3,)), dma, dma((2,)), dma((2,)), dma((3,)), dma((3, 3)), dma((3, 3)), dma((2,)), dma((3,)),
            dma, dma((C,)), dma, dma((C,)), dma, dma((C,)), dma, dma((C + 1,)),
        ]
        xo, qo, _ = pl.pallas_call(
            functools.partial(_kernel, T, C, float(d)),
            out_shape=(V((S, HL), BF16), V((S, QL), BF16), jax.ShapeDtypeStruct((2 * TP, 2, HL, NT), BF16)),
            in_specs=[any_] * 9,
            out_specs=(vm, vm, any_),
            scratch_shapes=scratch,
            compiler_params=pltpu.CompilerParams(collective_id=0, has_side_effects=True, vmem_limit_bytes=56 * 2**20),
            name='block',
        )(x, g1.reshape(1, HL), g2.reshape(1, HL), w_gate, w_up, w_down, o, w_o, w_qkv)
        return xo, qo

    in_specs = (P(None, 'h'), P('h'), P('h'), P('h', 'f'), P('h', 'f'), P('f', 'h'),
                P(None, 'f'), P('f', 'h'), P('h', 'f'))
    return jax.shard_map(body, mesh=mesh, in_specs=in_specs,
                         out_specs=(P(None, 'h'), P(None, 'f')), check_vma=False)
```

```python
import functools

import jax
import jax.numpy as jnp
from jax import lax
from jax.experimental import pallas as pl
from jax.experimental.pallas import tpu as pltpu
from jax.sharding import PartitionSpec as P

EPS = 1e-6
MESH = pl.DeviceIdType.MESH
F32 = jnp.float32
BF16 = jnp.bfloat16
NT = 256
NB = 3


def _dot(a, b):
    return jnp.dot(a, b, preferred_element_type=F32)


def _kernel(T, C, d,
            x_hbm, g1_hbm, g2_hbm, wg_hbm, wu_hbm, wd_hbm, o_hbm, wo_hbm, wq_hbm,
            xov, qall, wsib_hbm,
            xv, g1v, g2v, ov, wd, wo, wq, wbuf, nf, ss1, psnd, prcv, pkeep, abuf, ysnd, yrcv, ss2, nf2,
            qsnd, qrcv, qkeep,
            in_sem, ld_sem, w0_s, w0_r, ws_s, ws_r, wq_s, wq_r, n_s, n_r, ss1_s, ss1_r, p_s, p_r, a_s, a_r, y_s, y_r, ss2_s, ss2_r,
            n2_s, n2_r, q_s, q_r, qa_s, qa_r):
    S = xv.shape[0]
    HL = xv.shape[1]
    FB = abuf.shape[3]
    QB = qsnd.shape[2]
    TP = FB // NT
    QT = QB // NT
    DT = HL // NT
    f = lax.axis_index('f')
    h = lax.axis_index('h')
    c = lax.rem(h, 2)
    xx = h // 2
    hx = (1 - xx) * 2 + c
    hs = xx * 2 + (1 - c)
    hd = (1 - xx) * 2 + (1 - c)
    XP, SIB, DIAG, YP = (f, hx), (f, hs), (f, hd), (1 - f, h)

    def rcopy(src, dst, s, r, dev):
        return pltpu.make_async_remote_copy(src_ref=src, dst_ref=dst, send_sem=s, recv_sem=r, device_id=dev,
                                            device_id_type=MESH)

    def lcopy(src, dst, s):
        return pltpu.make_async_copy(src, dst, s)

    def lwait(ref, sem):
        lcopy(ref, ref, sem).wait()

    def rwait(ref, sem):
        rcopy(ref, ref, sem, sem, XP).wait_recv()

    def mo(v, m):
        return pl.multiple_of(v, m)

    top, rest = pl.ds(0, T), pl.ds(T, S - T)
    first = [lcopy(x_hbm.at[top], xv.at[top], in_sem.at[0]), lcopy(g1_hbm, g1v.at[:, pl.ds(0, HL)], in_sem.at[1])]
    second = [lcopy(x_hbm.at[rest], xv.at[rest], in_sem.at[2]), lcopy(g2_hbm, g2v, in_sem.at[7])]
    for cp in first:
        cp.start()

    bar = pltpu.get_barrier_semaphore()
    for dev in (XP, SIB, DIAG, YP):
        pl.semaphore_signal(bar, inc=1, device_id=dev, device_id_type=MESH)

    NL = 3 * TP + (C - 2) * 2 * TP

    def tile_of(g):
        return jnp.where(g < TP, g, lax.rem(g + TP, 2 * TP))

    def own(g):
        t = tile_of(g)
        bs = lax.rem(g, NB)
        blk = jnp.where(t < TP, hx, h)
        col = mo(blk * FB + lax.rem(t, TP) * NT, NT)
        return (lcopy(wg_hbm.at[:, pl.ds(col, NT)], wbuf.at[bs, 0, pl.ds(0, HL)], ld_sem.at[bs]),
                lcopy(wu_hbm.at[:, pl.ds(col, NT)], wbuf.at[bs, 1, pl.ds(0, HL)], ld_sem.at[bs]))

    def sib(g):
        t = tile_of(g)
        bs = lax.rem(g, NB)
        return (lcopy(wsib_hbm.at[t, 0], wbuf.at[bs, 0, pl.ds(HL, HL)], ld_sem.at[bs]),
                lcopy(wsib_hbm.at[t, 1], wbuf.at[bs, 1, pl.ds(HL, HL)], ld_sem.at[bs]))

    def wcopy(t, m):
        blk = jnp.where(t < TP, hd, hs)
        col = mo(blk * FB + lax.rem(t, TP) * NT, NT)
        src = (wg_hbm, wu_hbm)[m].at[:, pl.ds(col, NT)]
        return rcopy(src, wsib_hbm.at[t, m], ws_s, ws_r.at[t], SIB)

    def wqcopy(b, t):
        blk = (hd, hs)[b]
        col = mo(blk * QB + t * NT, NT)
        return rcopy(wq_hbm.at[:, pl.ds(col, NT)], wq.at[b, t, pl.ds(HL, HL)], wq_s, wq_r, SIB)

    def start_sib(g):
        @pl.when((g <= TP) | ((g >= 2 * TP) & (g < 3 * TP)))
        def _():
            t = tile_of(g)
            rwait(wsib_hbm.at[t], ws_r.at[t])

        for cp in sib(g):
            cp.start()

    def start_own(g):
        for cp in own(g):
            cp.start()

    def wait_tile(g):
        bs = lax.rem(g, NB)
        lwait(wbuf.at[bs], ld_sem.at[bs])

    start_own(jnp.int32(0))
    for cp in second:
        cp.start()
    start_own(jnp.int32(1))
    for cp in first:
        cp.wait()

    def row_sums(xf):
        s = jnp.broadcast_to(jnp.sum(xf * xf, axis=1, keepdims=True), (T, 128))
        if T < 128:
            s = jnp.concatenate([s] * (128 // T), axis=0)
        return s.T[0:1]

    def row_scales(ss):
        r = lax.rsqrt((ss[0] + ss[1] + ss[2] + ss[3]) / d + EPS)
        return jnp.broadcast_to(r, (128, 128)).T[0:T]

    def sums1(j):
        ss1[j, h] = row_sums(xv[pl.ds(j * T, T), :].astype(F32))

    sums1(0)

    def ss1copy(j, k):
        dev = (XP, SIB, DIAG)[k]
        return rcopy(ss1.at[j, h], ss1.at[j, h], ss1_s, ss1_r.at[min(j, 1)], dev)

    def xcopy(k):
        rows = (top, rest)[k]
        return rcopy(xv.at[rows], nf2.at[rows, pl.ds(HL, HL)], n_s.at[k], n_r.at[k], SIB)

    gcp = rcopy(g1v.at[:, pl.ds(0, HL)], g1v.at[:, pl.ds(HL, HL)], n_s.at[2], n_r.at[2], SIB)

    pl.semaphore_wait(bar, 4)
    for k in (0, 2, 1):
        ss1copy(0, k).start()
    xcopy(0).start()
    gcp.start()
    def w0copy(m):
        src = (wg_hbm, wu_hbm)[m].at[:, pl.ds(mo(hd * FB, NT), NT)]
        return rcopy(src, wbuf.at[0, m, pl.ds(HL, HL)], w0_s, w0_r, SIB)

    for m in range(2):
        w0copy(m).start()

    @pl.loop(1, TP)
    def _(t):
        for m in range(2):
            wcopy(t, m).start()

    for m in range(2):
        wcopy(jnp.int32(0), m).start()
    for cp in second:
        cp.wait()
    for j in range(1, C):
        sums1(j)
        for k in range(3):
            ss1copy(j, k).start()
    xcopy(1).start()

    @pl.loop(TP, 2 * TP)
    def _(t):
        for m in range(2):
            wcopy(t, m).start()

    for b in range(2):
        for t in range(QT):
            wqcopy(b, t).start()

    def norm1(j):
        if j == 0:
            rwait(ss1.at[0, pl.ds(0, 3)], ss1_r.at[0])
        elif j == 1:
            rwait(ss1.at[pl.ds(1, C - 1), pl.ds(0, 3)], ss1_r.at[1])
        rr = row_scales(ss1.at[j])
        rows = pl.ds(j * T, T)
        for half in range(2):
            for l in range(HL // 128):
                cols = pl.ds(half * HL + l * 128, 128)
                xb = xv[rows, pl.ds(l * 128, 128)] if half == 0 else nf2[rows, cols]
                nf[rows, cols] = (xb.astype(F32) * rr * g1v[:, cols]).astype(BF16)

    gcp.wait_recv()
    xcopy(0).wait_recv()
    norm1(0)

    def pcopy(j, t):
        s2 = lax.rem(j, 2)
        s3 = lax.rem(j, 3)
        return rcopy(psnd.at[s2, t], prcv.at[s3, t], p_s.at[s2], p_r.at[s3], XP)

    def gu(g, row, n):
        bs = lax.rem(g, NB)
        nn = nf[pl.ds(row, n), :]
        return _dot(nn, wbuf[bs, 0]), _dot(nn, wbuf[bs, 1])

    def prefetch(g):
        @pl.when(g < NL)
        def _():
            start_own(g)
            start_sib(g)

    def put_send(j, t, gg, uu):
        s2 = lax.rem(j, 2)
        psnd[s2, t, :, 0:NT] = gg
        psnd[s2, t, :, NT:2 * NT] = uu
        pcopy(j, t).start()

    def s12(j):
        s2 = lax.rem(j, 2)
        g0 = 3 * TP + (j - 2) * (2 * TP)
        rwait(psnd.at[s2], p_s.at[s2])
        row = mo(j * T, T)

        @pl.loop(0, TP)
        def _(t):
            wait_tile(g0 + t)
            prefetch(g0 + t + NB - 1)
            gg, uu = gu(g0 + t, row, T)
            put_send(j, t, gg, uu)

        @pl.loop(0, TP)
        def _(t):
            wait_tile(g0 + t + TP)
            prefetch(g0 + t + TP + NB - 1)
            gg, uu = gu(g0 + t + TP, row, T)
            pkeep[s2, t, :, 0:NT] = gg
            pkeep[s2, t, :, NT:2 * NT] = uu

    def acopy(i, k):
        sl = lax.rem(i, 3)
        b = (h, h, hx)[k]
        return rcopy(abuf.at[sl, b], abuf.at[sl, b], a_s.at[sl, k], a_r.at[sl, k], (XP, SIB, SIB)[k])

    def s3(i):
        s2 = lax.rem(i, 2)
        sl = lax.rem(i, 3)

        rwait(prcv.at[sl], p_r.at[sl])

        @pl.loop(0, TP)
        def _(t):
            gg = pkeep[s2, t, :, 0:NT] + prcv[sl, t, :, 0:NT]
            uu = pkeep[s2, t, :, NT:2 * NT] + prcv[sl, t, :, NT:2 * NT]
            abuf[sl, h, :, pl.ds(mo(t * NT, NT), NT)] = (gg * jax.nn.sigmoid(gg) * uu).astype(BF16)

        acopy(i, 0).start()
        acopy(i, 1).start()

    def ycopy(i, n):
        s2 = lax.rem(i, 2)
        cols = pl.ds(mo(n * NT, NT), NT)
        sl = lax.rem(i, 3)
        return rcopy(ysnd.at[s2, :, cols], yrcv.at[sl, :, cols], y_s.at[s2], y_r.at[sl], YP)

    def down(sl, b, n):
        return _dot(abuf[sl, b], wd[n, pl.ds(mo(b * FB, FB), FB)])

    def s4a(i):
        s2 = lax.rem(i, 2)
        sl = lax.rem(i, 3)
        acopy(i, 1).wait_recv()

        @pl.loop(0, DT)
        def _(n):
            acc = _dot(ov[pl.ds(mo(i * T, T), T), :], wo[n])
            acc += down(sl, h, n)
            acc += down(sl, hs, n)
            ysnd[s2, :, pl.ds(mo(n * NT, NT), NT)] = acc

    def s4b(i):
        s2 = lax.rem(i, 2)
        sl = lax.rem(i, 3)
        acopy(i, 0).wait_recv()
        acopy(i, 2).start()
        acopy(i, 2).wait_recv()

        @pl.loop(0, DT)
        def _(n):
            ysnd[s2, :, pl.ds(mo(n * NT, NT), NT)] += down(sl, hx, n) + down(sl, hd, n)
            ycopy(i, n).start()

    def ss2copy(i, k):
        dev = (XP, SIB, DIAG)[k]
        return rcopy(ss2.at[i, h], ss2.at[i, h], ss2_s, ss2_r.at[i], dev)

    def s5(i):
        s2 = lax.rem(i, 2)
        for k in range(3):
            acopy(i, k).wait_send()
        sl = lax.rem(i, 3)
        rwait(ysnd.at[s2], y_s.at[s2])
        rwait(yrcv.at[sl], y_r.at[sl])
        rows = pl.ds(mo(i * T, T), T)
        xn = (xv[rows, :].astype(F32) + (ysnd[s2] + yrcv[sl])).astype(BF16)
        xov[rows, :] = xn
        ss2[i, h] = row_sums(xn.astype(F32))
        for k in range(3):
            ss2copy(i, k).start()

    def n2copy(i):
        rows = pl.ds(mo(i * T, T), T)
        return rcopy(nf2.at[rows, pl.ds(0, HL)], nf2.at[rows, pl.ds(HL, HL)], n2_s, n2_r.at[i], SIB)

    def s6(i):
        rows = pl.ds(mo(i * T, T), T)
        rwait(ss2.at[i, pl.ds(0, 3)], ss2_r.at[i])
        rr = row_scales(ss2.at[i])
        for l in range(HL // 128):
            xf = xov[rows, pl.ds(l * 128, 128)].astype(F32)
            nf2[rows, pl.ds(l * 128, 128)] = (xf * rr * g2v[:, pl.ds(l * 128, 128)]).astype(BF16)
        n2copy(i).start()

    def qcopy(i):
        return rcopy(qsnd.at[i], qrcv.at[i], q_s, q_r.at[i], XP)

    def s7(i):
        n2copy(i).wait_recv()
        nn = nf2[pl.ds(mo(i * T, T), T), :]
        for t in range(QT):
            qsnd[i, :, t * NT:(t + 1) * NT] = _dot(nn, wq[0, t])
        qcopy(i).start()
        for t in range(QT):
            qkeep[i, :, t * NT:(t + 1) * NT] = _dot(nn, wq[1, t])

    def qacopy(i, k):
        b = (h, h, hx)[k]
        dev = (XP, SIB, SIB)[k]
        blk = qall.at[pl.ds(mo(i * T, T), T), pl.ds(mo(b * QB, NT), QB)]
        return rcopy(blk, blk, qa_s, qa_r.at[i if k == 0 else C], dev)

    def s8(i):
        qcopy(i).wait_recv()
        for t in range(QT):
            cols = pl.ds(t * NT, NT)
            qall[pl.ds(mo(i * T, T), T), pl.ds(mo(h * QB + t * NT, NT), NT)] = (qkeep[i, :, cols] + qrcv[i, :, cols]).astype(BF16)
        qacopy(i, 0).start()
        qacopy(i, 1).start()

    def s9a(i):
        qacopy(i, 0).wait_recv()
        qacopy(i, 2).start()

    lwait(wbuf.at[0, :, pl.ds(0, HL)], ld_sem.at[0])
    halves = [_dot(nf[top, pl.ds(0, HL)], wbuf[0, m, 0:HL]) for m in range(2)]
    rwait(wbuf.at[0, :, pl.ds(HL, HL)], w0_r)
    for m in range(2):
        cols = pl.ds(m * NT, NT)
        psnd[0, 0, :, cols] = halves[m] + _dot(nf[top, pl.ds(HL, HL)], wbuf[0, m, HL:2 * HL])
        rcopy(psnd.at[0, 0, :, cols], prcv.at[0, 0, :, cols], p_s.at[0], p_r.at[0], XP).start()
    start_own(jnp.int32(2))
    start_sib(jnp.int32(1))

    @pl.loop(1, TP)
    def _(t):
        wait_tile(t)
        gg, uu = gu(t, 0, T)
        put_send(jnp.int32(0), t, gg, uu)
        start_own(t + 2)
        start_sib(t + 1)

    start_sib(jnp.int32(TP + 1))
    xcopy(1).wait_recv()
    for j in range(1, C):
        norm1(j)

    @pl.loop(0, TP)
    def _(t):
        wait_tile(TP + t)
        prefetch(TP + t + NB - 1)
        gg, uu = gu(TP + t, T, T)
        put_send(jnp.int32(1), t, gg, uu)


    res = [[] for _ in range(4)]
    for n in range(DT):
        res[n % 4].append(lcopy(wd_hbm.at[:, pl.ds(n * NT, NT)], wd.at[n], in_sem.at[4]))
        res[n % 4].append(lcopy(wo_hbm.at[:, pl.ds(n * NT, NT)], wo.at[n], in_sem.at[5]))
    res[0].append(lcopy(o_hbm, ov, in_sem.at[3]))
    for b in range(2):
        blk = (hx, h)[b]
        for t in range(QT):
            res[3].append(lcopy(wq_hbm.at[:, pl.ds(mo(blk * QB + t * NT, NT), NT)], wq.at[b, t, pl.ds(0, HL)],
                                in_sem.at[6]))

    @pl.loop(0, TP)
    def _(t):
        wait_tile(2 * TP + t)
        prefetch(2 * TP + t + NB - 1)
        for k in range(4):
            @pl.when(t == k)
            def _(k=k):
                for cp in res[k]:
                    cp.start()

        gg, uu = gu(2 * TP + t, 0, 2 * T)
        for j in range(2):
            pkeep[j, t, :, 0:NT] = gg[j * T:(j + 1) * T]
            pkeep[j, t, :, NT:2 * NT] = uu[j * T:(j + 1) * T]

    def stage(fn, i, lo=0):
        @pl.when((i >= lo) & (i < C))
        def _():
            fn(i)

    def loaded():
        lwait(ov, in_sem.at[3])
        lwait(wd, in_sem.at[4])
        lwait(wo, in_sem.at[5])
        lwait(wq.at[:, :, pl.ds(0, HL)], in_sem.at[6])
        rwait(wq.at[:, :, pl.ds(HL, HL)], wq_s)
        rwait(wq.at[:, :, pl.ds(HL, HL)], wq_r)

    @pl.loop(0, C - 2)
    def _(i):
        s3(i)
        s12(i + 2)

        @pl.when(i == 0)
        def _():
            loaded()

        stage(s5, i - 1)
        s4a(i)
        s4b(i)
        stage(s6, i - 2)

    e = C - 1
    done = {s7: 0, s8: 0, s9a: 0}

    def run(*steps):
        for fn, i in steps:
            fn(jnp.int32(i))

    def nxt(*fns):
        for fn in fns:
            if done[fn] < C:
                fn(jnp.int32(done[fn]))
                done[fn] += 1

    run((s3, e - 1), (s4a, e - 1), (s5, e - 2), (s6, e - 3), (s3, e))
    nxt(s7)
    run((s4b, e - 1))
    nxt(s7)
    run((s4a, e), (s6, e - 2), (s4b, e))
    nxt(s7, s8)
    run((s5, e - 1))
    nxt(s7, s8)
    run((s5, e), (s6, e - 1))
    nxt(s7, s8)
    run((s6, e))
    nxt(s7, s8, s9a, s7, s8, s9a, s7, s8, s9a)
    gcp.wait_send()
    rwait(ss1.at[:, pl.ds(0, 3)], ss1_s)
    for k in range(2):
        xcopy(k).wait_send()

    rwait(wsib_hbm, ws_s)
    rwait(wbuf.at[0, :, pl.ds(HL, HL)], w0_s)

    for k in range(2):
        rwait(psnd.at[k], p_s.at[k])

    while done[s8] < C:
        nxt(s8, s9a)

    rwait(ss2.at[:, pl.ds(0, 3)], ss2_s)
    rwait(nf2.at[:, pl.ds(0, HL)], n2_s)
    rwait(qsnd, q_s)

    while done[s9a] < C:
        nxt(s9a)
    rwait(qall.at[:, pl.ds(0, 2 * QB)], qa_r.at[C])
    rwait(qall.at[:, pl.ds(0, 3 * QB)], qa_s)


def _out_kernel(xv, qv, xo, qo, sem):
    n = xv.shape[0] // 4
    cps = [pltpu.make_async_copy(a.at[pl.ds(k * n, n)], b.at[pl.ds(k * n, n)], sem.at[m, k])
           for m, (a, b) in enumerate(((qv, qo), (xv, xo))) for k in range(4)]
    for cp in cps:
        cp.start()
    for cp in cps:
        cp.wait()


def solution(mesh):
    nh = mesh.shape['h']

    def body(x, g1, g2, w_gate, w_up, w_down, o, w_o, w_qkv):
        S, HL = x.shape
        FL = w_gate.shape[1]
        FB = FL // nh
        QL = w_qkv.shape[1]
        QB = QL // nh
        OL = o.shape[1]
        T = 64
        C = S // T
        TP, QT, DT = FB // NT, QB // NT, HL // NT
        d = HL * nh
        any_ = pl.BlockSpec(memory_space=pl.ANY)
        vm = pl.BlockSpec(memory_space=pltpu.VMEM)
        dma = pltpu.SemaphoreType.DMA
        V = pltpu.VMEM
        scratch = [
            V((S, HL), BF16), V((1, 2 * HL), F32), V((1, HL), F32), V((S, OL), BF16),
            V((DT, FL, NT), BF16), V((DT, OL, NT), BF16), V((2, QT, 2 * HL, NT), BF16),
            V((NB, 2, 2 * HL, NT), BF16), V((S, 2 * HL), BF16), V((C, nh, 1, 128), F32),
            V((2, TP, T, 2 * NT), F32), V((3, TP, T, 2 * NT), F32), V((2, TP, T, 2 * NT), F32),
            V((3, nh, T, FB), BF16), V((2, T, HL), F32), V((3, T, HL), F32),
            V((C, nh, 1, 128), F32), V((S, 2 * HL), BF16),
            V((C, T, QB), F32), V((C, T, QB), F32), V((C, T, QB), F32),
            dma((8,)), dma((NB,)), dma, dma, dma, dma((2 * TP,)), dma, dma,
            dma((3,)), dma((3,)), dma, dma((2,)), dma((2,)), dma((3,)), dma((3, 3)), dma((3, 3)), dma((2,)), dma((3,)),
            dma, dma((C,)), dma, dma((C,)), dma, dma((C,)), dma, dma((C + 1,)),
        ]
        xo, qo, _ = pl.pallas_call(
            functools.partial(_kernel, T, C, float(d)),
            out_shape=(V((S, HL), BF16), V((S, QL), BF16), jax.ShapeDtypeStruct((2 * TP, 2, HL, NT), BF16)),
            in_specs=[any_] * 9,
            out_specs=(vm, vm, any_),
            scratch_shapes=scratch,
            compiler_params=pltpu.CompilerParams(collective_id=0, has_side_effects=True, vmem_limit_bytes=56 * 2**20),
            name='block',
        )(x, g1.reshape(1, HL), g2.reshape(1, HL), w_gate, w_up, w_down, o, w_o, w_qkv)
        return pl.pallas_call(
            _out_kernel,
            out_shape=(jax.ShapeDtypeStruct((S, HL), BF16), jax.ShapeDtypeStruct((S, QL), BF16)),
            in_specs=[vm, vm],
            out_specs=(any_, any_),
            scratch_shapes=[dma((2, 4))],
            compiler_params=pltpu.CompilerParams(vmem_limit_bytes=2**20),
            name='out',
        )(xo, qo)

    in_specs = (P(None, 'h'), P('h'), P('h'), P('h', 'f'), P('h', 'f'), P('f', 'h'),
                P(None, 'f'), P('f', 'h'), P('h', 'f'))
    return jax.shard_map(body, mesh=mesh, in_specs=in_specs,
                         out_specs=(P(None, 'h'), P(None, 'f')), check_vma=False)
```

```python
import functools

import jax
import jax.numpy as jnp
from jax import lax
from jax.experimental import pallas as pl
from jax.experimental.pallas import tpu as pltpu
from jax.sharding import PartitionSpec as P

EPS = 1e-6
MESH = pl.DeviceIdType.MESH
F32 = jnp.float32
BF16 = jnp.bfloat16
NT = 256
NB = 3
HOLD = 2


def _dot(a, b):
    return jnp.dot(a, b, preferred_element_type=F32)


def _kernel(T, C, d,
            x_hbm, g1_hbm, g2_hbm, wg_hbm, wu_hbm, wd_hbm, o_hbm, wo_hbm, wq_hbm,
            xov, qall, wsib_hbm,
            xv, g1v, g2v, ov, wd, wo, wq, wbuf, nf, ss1, psnd, prcv, pkeep, abuf, ysnd, yrcv, ss2, nf2,
            qsnd, qrcv, qkeep,
            in_sem, ld_sem, w0_s, w0_r, ws_s, ws_r, wq_s, wq_r, n_s, n_r, ss1_s, ss1_r, p_s, p_r, a_s, a_r, y_s, y_r, ss2_s, ss2_r,
            n2_s, n2_r, q_s, q_r, qa_s, qa_r):
    S = xv.shape[0]
    HL = xv.shape[1]
    FB = abuf.shape[3]
    QB = qsnd.shape[2]
    TP = FB // NT
    QT = QB // NT
    DT = HL // NT
    f = lax.axis_index('f')
    h = lax.axis_index('h')
    c = lax.rem(h, 2)
    xx = h // 2
    hx = (1 - xx) * 2 + c
    hs = xx * 2 + (1 - c)
    hd = (1 - xx) * 2 + (1 - c)
    XP, SIB, DIAG, YP = (f, hx), (f, hs), (f, hd), (1 - f, h)

    def rcopy(src, dst, s, r, dev):
        return pltpu.make_async_remote_copy(src_ref=src, dst_ref=dst, send_sem=s, recv_sem=r, device_id=dev,
                                            device_id_type=MESH)

    def lcopy(src, dst, s):
        return pltpu.make_async_copy(src, dst, s)

    def lwait(ref, sem):
        lcopy(ref, ref, sem).wait()

    def rwait(ref, sem):
        rcopy(ref, ref, sem, sem, XP).wait_recv()

    def mo(v, m):
        return pl.multiple_of(v, m)

    top, rest = pl.ds(0, T), pl.ds(T, S - T)
    first = [lcopy(x_hbm.at[top], xv.at[top], in_sem.at[0]), lcopy(g1_hbm, g1v.at[:, pl.ds(0, HL)], in_sem.at[1])]
    second = [lcopy(x_hbm.at[rest], xv.at[rest], in_sem.at[2]), lcopy(g2_hbm, g2v, in_sem.at[3])]
    for cp in first:
        cp.start()

    bar = pltpu.get_barrier_semaphore()
    for dev in (XP, SIB, DIAG, YP):
        pl.semaphore_signal(bar, inc=1, device_id=dev, device_id_type=MESH)

    NL = 3 * TP + (C - 2) * 2 * TP

    def tile_of(g):
        return jnp.where(g < TP, g, lax.rem(g + TP, 2 * TP))

    def own(g):
        t = tile_of(g)
        bs = lax.rem(g, NB)
        blk = jnp.where(t < TP, hx, h)
        col = mo(blk * FB + lax.rem(t, TP) * NT, NT)
        return (lcopy(wg_hbm.at[:, pl.ds(col, NT)], wbuf.at[bs, 0, pl.ds(0, HL)], ld_sem.at[bs]),
                lcopy(wu_hbm.at[:, pl.ds(col, NT)], wbuf.at[bs, 1, pl.ds(0, HL)], ld_sem.at[bs]))

    def sib(g):
        t = tile_of(g)
        bs = lax.rem(g, NB)
        return (lcopy(wsib_hbm.at[t, 0], wbuf.at[bs, 0, pl.ds(HL, HL)], ld_sem.at[bs]),
                lcopy(wsib_hbm.at[t, 1], wbuf.at[bs, 1, pl.ds(HL, HL)], ld_sem.at[bs]))

    def wcopy(t, m):
        blk = jnp.where(t < TP, hd, hs)
        col = mo(blk * FB + lax.rem(t, TP) * NT, NT)
        src = (wg_hbm, wu_hbm)[m].at[:, pl.ds(col, NT)]
        return rcopy(src, wsib_hbm.at[t, m], ws_s, ws_r.at[t], SIB)

    def wqcopy(b, t):
        blk = (hd, hs)[b]
        col = mo(blk * QB + t * NT, NT)
        return rcopy(wq_hbm.at[:, pl.ds(col, NT)], wq.at[b, t, pl.ds(HL, HL)], wq_s, wq_r, SIB)

    def start_sib(g):
        @pl.when((g <= TP) | ((g >= 2 * TP) & (g < 3 * TP)))
        def _():
            t = tile_of(g)
            rwait(wsib_hbm.at[t], ws_r.at[t])

        for cp in sib(g):
            cp.start()

    def start_own(g):
        for cp in own(g):
            cp.start()

    def wait_tile(g):
        bs = lax.rem(g, NB)
        lwait(wbuf.at[bs], ld_sem.at[bs])

    first[0].wait()
    start_own(jnp.int32(0))
    for cp in second:
        cp.start()
    start_own(jnp.int32(1))

    def row_sums(xf):
        s = jnp.broadcast_to(jnp.sum(xf * xf, axis=1, keepdims=True), (T, 128))
        if T < 128:
            s = jnp.concatenate([s] * (128 // T), axis=0)
        return s.T[0:1]

    def row_scales(ss):
        r = lax.rsqrt((ss[0] + ss[1] + ss[2] + ss[3]) / d + EPS)
        return jnp.broadcast_to(r, (128, 128)).T[0:T]

    def sums1(j):
        ss1[j, h] = row_sums(xv[pl.ds(j * T, T), :].astype(F32))

    sums1(0)

    def ss1copy(j, k):
        dev = (XP, SIB, DIAG)[k]
        return rcopy(ss1.at[j, h], ss1.at[j, h], ss1_s, ss1_r.at[min(j, 1)], dev)

    def xcopy(k):
        rows = (top, rest)[k]
        return rcopy(xv.at[rows], nf2.at[rows, pl.ds(HL, HL)], n_s.at[k], n_r.at[k], SIB)

    gcp = rcopy(g1v.at[:, pl.ds(0, HL)], g1v.at[:, pl.ds(HL, HL)], n_s.at[2], n_r.at[2], SIB)

    first[1].wait()
    pl.semaphore_wait(bar, 4)
    for k in (0, 2, 1):
        ss1copy(0, k).start()
    xcopy(0).start()
    gcp.start()
    def w0copy(m):
        src = (wg_hbm, wu_hbm)[m].at[:, pl.ds(mo(hd * FB, NT), NT)]
        return rcopy(src, wbuf.at[0, m, pl.ds(HL, HL)], w0_s, w0_r.at[m], SIB)

    for m in range(2):
        w0copy(m).start()

    @pl.loop(1, TP)
    def _(t):
        for m in range(2):
            wcopy(t, m).start()

    for m in range(2):
        wcopy(jnp.int32(0), m).start()
    for cp in second:
        cp.wait()
    for j in range(1, C):
        sums1(j)
        for k in range(3):
            ss1copy(j, k).start()
    xcopy(1).start()

    @pl.loop(TP, 2 * TP)
    def _(t):
        for m in range(2):
            wcopy(t, m).start()

    for b in range(2):
        for t in range(QT):
            wqcopy(b, t).start()

    def norm1(j):
        if j == 0:
            rwait(ss1.at[0, pl.ds(0, 3)], ss1_r.at[0])
        elif j == 1:
            rwait(ss1.at[pl.ds(1, C - 1), pl.ds(0, 3)], ss1_r.at[1])
        rr = row_scales(ss1.at[j])
        rows = pl.ds(j * T, T)
        for half in range(2):
            for l in range(HL // 128):
                cols = pl.ds(half * HL + l * 128, 128)
                xb = xv[rows, pl.ds(l * 128, 128)] if half == 0 else nf2[rows, cols]
                nf[rows, cols] = (xb.astype(F32) * rr * g1v[:, cols]).astype(BF16)

    gcp.wait_recv()
    xcopy(0).wait_recv()
    norm1(0)

    def pcopy(j, t):
        s2 = lax.rem(j, 2)
        s3 = lax.rem(j, 3)
        return rcopy(psnd.at[s2, t], prcv.at[s3, t], p_s.at[s2], p_r.at[s3], XP)

    def gu(g, row, n):
        bs = lax.rem(g, NB)
        nn = nf[pl.ds(row, n), :]
        return _dot(nn, wbuf[bs, 0]), _dot(nn, wbuf[bs, 1])

    def prefetch(g):
        @pl.when(g < NL)
        def _():
            start_own(g)
            start_sib(g)

    def put_send(j, t, gg, uu):
        s2 = lax.rem(j, 2)
        psnd[s2, t, :, 0:NT] = gg
        psnd[s2, t, :, NT:2 * NT] = uu
        pcopy(j, t).start()

    def s12(j):
        s2 = lax.rem(j, 2)
        g0 = 3 * TP + (j - 2) * (2 * TP)
        rwait(psnd.at[s2], p_s.at[s2])
        row = mo(j * T, T)

        @pl.loop(0, TP)
        def _(t):
            wait_tile(g0 + t)
            prefetch(g0 + t + NB - 1)
            gg, uu = gu(g0 + t, row, T)
            put_send(j, t, gg, uu)

        @pl.loop(0, TP)
        def _(t):
            wait_tile(g0 + t + TP)
            prefetch(g0 + t + TP + NB - 1)
            gg, uu = gu(g0 + t + TP, row, T)
            pkeep[s2, t, :, 0:NT] = gg
            pkeep[s2, t, :, NT:2 * NT] = uu

    def acopy(i, k):
        sl = lax.rem(i, 3)
        b = (h, h, hx)[k]
        return rcopy(abuf.at[sl, b], abuf.at[sl, b], a_s.at[sl], a_r.at[sl, k], (XP, SIB, SIB)[k])

    def s3(i):
        s2 = lax.rem(i, 2)
        sl = lax.rem(i, 3)

        rwait(prcv.at[sl], p_r.at[sl])

        @pl.loop(0, TP)
        def _(t):
            gg = pkeep[s2, t, :, 0:NT] + prcv[sl, t, :, 0:NT]
            uu = pkeep[s2, t, :, NT:2 * NT] + prcv[sl, t, :, NT:2 * NT]
            abuf[sl, h, :, pl.ds(mo(t * NT, NT), NT)] = (gg * jax.nn.sigmoid(gg) * uu).astype(BF16)

        acopy(i, 0).start()
        acopy(i, 1).start()

    def ycopy(i, n):
        s2 = lax.rem(i, 2)
        cols = pl.ds(mo(n * NT, NT), NT)
        sl = lax.rem(i, 3)
        return rcopy(ysnd.at[s2, :, cols], yrcv.at[sl, :, cols], y_s.at[s2], y_r.at[sl], YP)

    def down(sl, b, n):
        return _dot(abuf[sl, b], wd[n, pl.ds(mo(b * FB, FB), FB)])

    def s4a(i):
        s2 = lax.rem(i, 2)
        sl = lax.rem(i, 3)
        acopy(i, 1).wait_recv()

        @pl.loop(0, DT)
        def _(n):
            acc = _dot(ov[pl.ds(mo(i * T, T), T), :], wo[n])
            acc += down(sl, h, n)
            acc += down(sl, hs, n)
            ysnd[s2, :, pl.ds(mo(n * NT, NT), NT)] = acc

    def s4b(i):
        s2 = lax.rem(i, 2)
        sl = lax.rem(i, 3)
        acopy(i, 0).wait_recv()
        acopy(i, 2).start()
        acopy(i, 2).wait_recv()

        @pl.loop(0, DT)
        def _(n):
            ysnd[s2, :, pl.ds(mo(n * NT, NT), NT)] += down(sl, hx, n) + down(sl, hd, n)
            ycopy(i, n).start()

    def ss2copy(i, k):
        dev = (XP, SIB, DIAG)[k]
        return rcopy(ss2.at[i, h], ss2.at[i, h], ss2_s, ss2_r.at[lax.rem(i, 4)], dev)

    def s5(i):
        s2 = lax.rem(i, 2)
        sl = lax.rem(i, 3)
        rwait(abuf.at[sl, pl.ds(0, 3)], a_s.at[sl])
        rwait(ysnd.at[s2], y_s.at[s2])
        rwait(yrcv.at[sl], y_r.at[sl])
        rows = pl.ds(mo(i * T, T), T)
        xn = (xv[rows, :].astype(F32) + (ysnd[s2] + yrcv[sl])).astype(BF16)
        xov[rows, :] = xn
        ss2[i, h] = row_sums(xn.astype(F32))
        for k in range(3):
            ss2copy(i, k).start()

    def n2copy(i):
        rows = pl.ds(mo(i * T, T), T)
        return rcopy(nf2.at[rows, pl.ds(0, HL)], nf2.at[rows, pl.ds(HL, HL)], n2_s, n2_r.at[i], SIB)

    def s6(i):
        rows = pl.ds(mo(i * T, T), T)
        rwait(ss2.at[i, pl.ds(0, 3)], ss2_r.at[lax.rem(i, 4)])
        rr = row_scales(ss2.at[i])
        for l in range(HL // 128):
            xf = xov[rows, pl.ds(l * 128, 128)].astype(F32)
            nf2[rows, pl.ds(l * 128, 128)] = (xf * rr * g2v[:, pl.ds(l * 128, 128)]).astype(BF16)
        n2copy(i).start()

    def qcopy(i):
        return rcopy(qsnd.at[i], qrcv.at[i], q_s, q_r.at[i], XP)

    def s7(i):
        n2copy(i).wait_recv()
        nn = nf2[pl.ds(mo(i * T, T), T), :]
        for t in range(QT):
            qsnd[i, :, t * NT:(t + 1) * NT] = _dot(nn, wq[0, t])
        qcopy(i).start()
        for t in range(QT):
            qkeep[i, :, t * NT:(t + 1) * NT] = _dot(nn, wq[1, t])

    def qacopy(i, k):
        b = (h, h, hx)[k]
        dev = (XP, SIB, SIB)[k]
        blk = qall.at[pl.ds(mo(i * T, T), T), pl.ds(mo(b * QB, NT), QB)]
        return rcopy(blk, blk, qa_s, qa_r.at[i if k == 0 else C], dev)

    def s8(i, late=False):
        qcopy(i).wait_recv()
        for t in range(QT):
            cols = pl.ds(t * NT, NT)
            qall[pl.ds(mo(i * T, T), T), pl.ds(mo(h * QB + t * NT, NT), NT)] = (qkeep[i, :, cols] + qrcv[i, :, cols]).astype(BF16)
        qacopy(i, 1).start()
        if late:
            pl.when(c == 0)(qacopy(i, 0).start)
        else:
            qacopy(i, 0).start()

    def s9a(i):
        qacopy(i, 0).wait_recv()
        qacopy(i, 2).start()

    lwait(wbuf.at[0, :, pl.ds(0, HL)], ld_sem.at[0])
    for m in range(2):
        cols = pl.ds(m * NT, NT)
        rwait(wbuf.at[0, m, pl.ds(HL, HL)], w0_r.at[m])
        psnd[0, 0, :, cols] = _dot(nf[top, :], wbuf[0, m])
        rcopy(psnd.at[0, 0, :, cols], prcv.at[0, 0, :, cols], p_s.at[0], p_r.at[0], XP).start()
    start_own(jnp.int32(2))
    start_sib(jnp.int32(1))

    @pl.loop(1, TP)
    def _(t):
        wait_tile(t)
        gg, uu = gu(t, 0, T)
        put_send(jnp.int32(0), t, gg, uu)
        start_own(t + 2)
        start_sib(t + 1)

    start_sib(jnp.int32(TP + 1))
    xcopy(1).wait_recv()
    for j in range(1, C):
        norm1(j)

    @pl.loop(0, TP)
    def _(t):
        wait_tile(TP + t)
        prefetch(TP + t + NB - 1)
        gg, uu = gu(TP + t, T, T)
        put_send(jnp.int32(1), t, gg, uu)


    res = [[] for _ in range(4)]
    for n in range(DT):
        res[n % 4].append(lcopy(wd_hbm.at[:, pl.ds(n * NT, NT)], wd.at[n], in_sem.at[1]))
        res[n % 4].append(lcopy(wo_hbm.at[:, pl.ds(n * NT, NT)], wo.at[n], in_sem.at[2]))
    res[0].append(lcopy(o_hbm, ov, in_sem.at[0]))
    for b in range(2):
        blk = (hx, h)[b]
        for t in range(QT):
            res[3].append(lcopy(wq_hbm.at[:, pl.ds(mo(blk * QB + t * NT, NT), NT)], wq.at[b, t, pl.ds(0, HL)],
                                in_sem.at[3]))

    @pl.loop(0, TP)
    def _(t):
        wait_tile(2 * TP + t)
        prefetch(2 * TP + t + NB - 1)
        for k in range(4):
            @pl.when(t == k)
            def _(k=k):
                for cp in res[k]:
                    cp.start()

        gg, uu = gu(2 * TP + t, 0, 2 * T)
        for j in range(2):
            pkeep[j, t, :, 0:NT] = gg[j * T:(j + 1) * T]
            pkeep[j, t, :, NT:2 * NT] = uu[j * T:(j + 1) * T]

    def stage(fn, i, lo=0):
        @pl.when((i >= lo) & (i < C))
        def _():
            fn(i)

    def loaded():
        lwait(ov, in_sem.at[0])
        lwait(wd, in_sem.at[1])
        lwait(wo, in_sem.at[2])
        lwait(wq.at[:, :, pl.ds(0, HL)], in_sem.at[3])
        rwait(wq.at[:, :, pl.ds(HL, HL)], wq_s)
        rwait(wq.at[:, :, pl.ds(HL, HL)], wq_r)

    @pl.loop(0, C - 2)
    def _(i):
        s3(i)
        s12(i + 2)

        @pl.when(i == 0)
        def _():
            loaded()

        stage(s5, i - 1)
        s4a(i)
        s4b(i)
        stage(s6, i - 2)

    e = C - 1
    done = {s7: 0, s8: 0, s9a: 0}

    def run(*steps):
        for fn, i in steps:
            fn(jnp.int32(i))

    def nxt(*fns):
        for fn in fns:
            if done[fn] < C:
                fn(jnp.int32(done[fn]))
                done[fn] += 1

    run((s3, e - 1), (s4a, e - 1), (s5, e - 2), (s6, e - 3), (s3, e))
    nxt(s7)
    run((s4b, e - 1))
    nxt(s7)
    run((s4a, e), (s6, e - 2), (s4b, e))
    nxt(s7, s8)
    run((s5, e - 1))
    nxt(s7, s8)
    run((s5, e), (s6, e - 1))
    nxt(s7, s8)
    run((s6, e))
    nxt(s7, s8, s9a, s7, s8, s9a, s7, s9a)
    gcp.wait_send()
    rwait(ss1.at[:, pl.ds(0, 3)], ss1_s)
    for k in range(2):
        xcopy(k).wait_send()

    rwait(wsib_hbm, ws_s)
    rwait(wbuf.at[0, :, pl.ds(HL, HL)], w0_s)

    for k in range(2):
        rwait(psnd.at[k], p_s.at[k])

    while done[s8] < C - HOLD - 1:
        nxt(s8, s9a)
    while done[s8] < C - 1:
        s8(jnp.int32(done[s8]), late=True)
        done[s8] += 1
        if done[s9a] < C - HOLD - 1:
            nxt(s9a)

    s8(jnp.int32(C - 1), late=True)

    @pl.when(c == 1)
    def _():
        for i in range(C - HOLD - 1, C):
            qacopy(jnp.int32(i), 0).start()

    rwait(ss2.at[:, pl.ds(0, 3)], ss2_s)
    rwait(nf2.at[:, pl.ds(0, HL)], n2_s)
    rwait(qsnd, q_s)

    while done[s9a] < C:
        nxt(s9a)
    rwait(qall.at[:, pl.ds(0, 2 * QB)], qa_r.at[C])
    rwait(qall.at[:, pl.ds(0, 3 * QB)], qa_s)


def _out_kernel(xv, qv, xo, qo, sem):
    n = xv.shape[0] // 4
    cps = [pltpu.make_async_copy(a.at[pl.ds(k * n, n)], b.at[pl.ds(k * n, n)], sem.at[m, k])
           for m, (a, b) in enumerate(((qv, qo), (xv, xo))) for k in range(4)]
    for cp in cps:
        cp.start()
    for cp in cps:
        cp.wait()


def solution(mesh):
    nh = mesh.shape['h']

    def body(x, g1, g2, w_gate, w_up, w_down, o, w_o, w_qkv):
        S, HL = x.shape
        FL = w_gate.shape[1]
        FB = FL // nh
        QL = w_qkv.shape[1]
        QB = QL // nh
        OL = o.shape[1]
        T = 64
        C = S // T
        TP, QT, DT = FB // NT, QB // NT, HL // NT
        d = HL * nh
        any_ = pl.BlockSpec(memory_space=pl.ANY)
        vm = pl.BlockSpec(memory_space=pltpu.VMEM)
        dma = pltpu.SemaphoreType.DMA
        V = pltpu.VMEM
        scratch = [
            V((S, HL), BF16), V((1, 2 * HL), F32), V((1, HL), F32), V((S, OL), BF16),
            V((DT, FL, NT), BF16), V((DT, OL, NT), BF16), V((2, QT, 2 * HL, NT), BF16),
            V((NB, 2, 2 * HL, NT), BF16), V((S, 2 * HL), BF16), V((C, nh, 1, 128), F32),
            V((2, TP, T, 2 * NT), F32), V((3, TP, T, 2 * NT), F32), V((2, TP, T, 2 * NT), F32),
            V((3, nh, T, FB), BF16), V((2, T, HL), F32), V((3, T, HL), F32),
            V((C, nh, 1, 128), F32), V((S, 2 * HL), BF16),
            V((C, T, QB), F32), V((C, T, QB), F32), V((C, T, QB), F32),
            dma((4,)), dma((NB,)), dma, dma((2,)), dma, dma((2 * TP,)), dma, dma,
            dma((3,)), dma((3,)), dma, dma((2,)), dma((2,)), dma((3,)), dma((3,)), dma((3, 3)), dma((2,)), dma((3,)),
            dma, dma((4,)), dma, dma((C,)), dma, dma((C,)), dma, dma((C + 1,)),
        ]
        xo, qo, _ = pl.pallas_call(
            functools.partial(_kernel, T, C, float(d)),
            out_shape=(V((S, HL), BF16), V((S, QL), BF16), jax.ShapeDtypeStruct((2 * TP, 2, HL, NT), BF16)),
            in_specs=[any_] * 9,
            out_specs=(vm, vm, any_),
            scratch_shapes=scratch,
            compiler_params=pltpu.CompilerParams(collective_id=0, has_side_effects=True, vmem_limit_bytes=56 * 2**20),
            name='block',
        )(x, g1.reshape(1, HL), g2.reshape(1, HL), w_gate, w_up, w_down, o, w_o, w_qkv)
        return pl.pallas_call(
            _out_kernel,
            out_shape=(jax.ShapeDtypeStruct((S, HL), BF16), jax.ShapeDtypeStruct((S, QL), BF16)),
            in_specs=[vm, vm],
            out_specs=(any_, any_),
            scratch_shapes=[dma((2, 4))],
            compiler_params=pltpu.CompilerParams(vmem_limit_bytes=2**20),
            name='out',
        )(xo, qo)

    in_specs = (P(None, 'h'), P('h'), P('h'), P('h', 'f'), P('h', 'f'), P('f', 'h'),
                P(None, 'f'), P('f', 'h'), P('h', 'f'))
    return jax.shard_map(body, mesh=mesh, in_specs=in_specs,
                         out_specs=(P(None, 'h'), P(None, 'f')), check_vma=False)
```

```python
import functools

import jax
import jax.numpy as jnp
from jax import lax
from jax.experimental import pallas as pl
from jax.experimental.pallas import tpu as pltpu
from jax.sharding import PartitionSpec as P

EPS = 1e-6
MESH = pl.DeviceIdType.MESH
F32 = jnp.float32
BF16 = jnp.bfloat16
NT = 256
NB = 4
HOLD = 2


def _dot(a, b):
    return jnp.dot(a, b, preferred_element_type=F32)


def _kernel(T, C, d,
            x_hbm, g1_hbm, g2_hbm, wg_hbm, wu_hbm, wd_hbm, o_hbm, wo_hbm, wq_hbm,
            xov, qall, wsib_hbm,
            xv, g1v, g2v, ov, wd, wo, wq, wbuf, nf, ss1, psnd, prcv, pkeep, abuf, ysnd, yrcv, ss2, nf2,
            qsnd, qrcv, qkeep,
            in_sem, ld_sem, w0_s, w0_r, ws_s, ws_r, wq_s, wq_r, n_s, n_r, ss1_s, ss1_r, p_s, p_r, a_s, a_r, y_s, y_r, ss2_s, ss2_r,
            n2_s, n2_r, q_s, q_r, qa_s, qa_r):
    S = xv.shape[0]
    HL = xv.shape[1]
    FB = abuf.shape[3]
    QB = qsnd.shape[2]
    TP = FB // NT
    QT = QB // NT
    DT = HL // NT
    f = lax.axis_index('f')
    h = lax.axis_index('h')
    c = lax.rem(h, 2)
    xx = h // 2
    hx = (1 - xx) * 2 + c
    hs = xx * 2 + (1 - c)
    hd = (1 - xx) * 2 + (1 - c)
    XP, SIB, DIAG, YP = (f, hx), (f, hs), (f, hd), (1 - f, h)

    def rcopy(src, dst, s, r, dev):
        return pltpu.make_async_remote_copy(src_ref=src, dst_ref=dst, send_sem=s, recv_sem=r, device_id=dev,
                                            device_id_type=MESH)

    def lcopy(src, dst, s):
        return pltpu.make_async_copy(src, dst, s)

    def lwait(ref, sem):
        lcopy(ref, ref, sem).wait()

    def rwait(ref, sem):
        rcopy(ref, ref, sem, sem, XP).wait_recv()

    def mo(v, m):
        return pl.multiple_of(v, m)

    top, rest = pl.ds(0, T), pl.ds(T, S - T)
    first = [lcopy(x_hbm.at[top], xv.at[top], in_sem.at[0]), lcopy(g1_hbm, g1v.at[:, pl.ds(0, HL)], in_sem.at[1])]
    second = [lcopy(x_hbm.at[rest], xv.at[rest], in_sem.at[2]), lcopy(g2_hbm, g2v, in_sem.at[3])]
    for cp in first:
        cp.start()

    bar = pltpu.get_barrier_semaphore()
    for dev in (XP, SIB, DIAG, YP):
        pl.semaphore_signal(bar, inc=1, device_id=dev, device_id_type=MESH)

    NL = 3 * TP + (C - 2) * 2 * TP

    def tile_of(g):
        return jnp.where(g < TP, g, lax.rem(g + TP, 2 * TP))

    def own(g):
        t = tile_of(g)
        bs = lax.rem(g, NB)
        blk = jnp.where(t < TP, hx, h)
        col = mo(blk * FB + lax.rem(t, TP) * NT, NT)
        return (lcopy(wg_hbm.at[:, pl.ds(col, NT)], wbuf.at[bs, 0, pl.ds(0, HL)], ld_sem.at[bs]),
                lcopy(wu_hbm.at[:, pl.ds(col, NT)], wbuf.at[bs, 1, pl.ds(0, HL)], ld_sem.at[bs]))

    def sib(g):
        t = tile_of(g)
        bs = lax.rem(g, NB)
        return (lcopy(wsib_hbm.at[t, 0], wbuf.at[bs, 0, pl.ds(HL, HL)], ld_sem.at[bs]),
                lcopy(wsib_hbm.at[t, 1], wbuf.at[bs, 1, pl.ds(HL, HL)], ld_sem.at[bs]))

    def wcopy(t, m):
        blk = jnp.where(t < TP, hd, hs)
        col = mo(blk * FB + lax.rem(t, TP) * NT, NT)
        src = (wg_hbm, wu_hbm)[m].at[:, pl.ds(col, NT)]
        return rcopy(src, wsib_hbm.at[t, m], ws_s, ws_r.at[t], SIB)

    def wqcopy(b, t):
        blk = (hd, hs)[b]
        col = mo(blk * QB + t * NT, NT)
        return rcopy(wq_hbm.at[:, pl.ds(col, NT)], wq.at[b, t, pl.ds(HL, HL)], wq_s, wq_r, SIB)

    def start_sib(g):
        @pl.when((g <= TP) | ((g >= 2 * TP) & (g < 3 * TP)))
        def _():
            t = tile_of(g)
            rwait(wsib_hbm.at[t], ws_r.at[t])

        for cp in sib(g):
            cp.start()

    def start_own(g):
        for cp in own(g):
            cp.start()

    def wait_tile(g):
        bs = lax.rem(g, NB)
        lwait(wbuf.at[bs], ld_sem.at[bs])

    first[0].wait()
    start_own(jnp.int32(0))
    for cp in second:
        cp.start()
    start_own(jnp.int32(1))

    def row_sums(xf):
        s = jnp.broadcast_to(jnp.sum(xf * xf, axis=1, keepdims=True), (T, 128))
        if T < 128:
            s = jnp.concatenate([s] * (128 // T), axis=0)
        return s.T[0:1]

    def row_scales(ss):
        r = lax.rsqrt((ss[0] + ss[1] + ss[2] + ss[3]) / d + EPS)
        return jnp.broadcast_to(r, (128, 128)).T[0:T]

    def sums1(j):
        ss1[j, h] = row_sums(xv[pl.ds(j * T, T), :].astype(F32))

    sums1(0)

    def ss1copy(j, k):
        dev = (XP, SIB, DIAG)[k]
        return rcopy(ss1.at[j, h], ss1.at[j, h], ss1_s, ss1_r.at[min(j, 1)], dev)

    def xcopy(k):
        rows = (top, rest)[k]
        return rcopy(xv.at[rows], nf2.at[rows, pl.ds(HL, HL)], n_s.at[k], n_r.at[k], SIB)

    gcp = rcopy(g1v.at[:, pl.ds(0, HL)], g1v.at[:, pl.ds(HL, HL)], n_s.at[2], n_r.at[2], SIB)

    first[1].wait()
    pl.semaphore_wait(bar, 4)
    for k in (0, 2, 1):
        ss1copy(0, k).start()
    xcopy(0).start()
    gcp.start()
    def w0copy(m):
        src = (wg_hbm, wu_hbm)[m].at[:, pl.ds(mo(hd * FB, NT), NT)]
        return rcopy(src, wbuf.at[0, m, pl.ds(HL, HL)], w0_s, w0_r.at[m], SIB)

    for m in range(2):
        w0copy(m).start()

    @pl.loop(1, TP)
    def _(t):
        for m in range(2):
            wcopy(t, m).start()

    for m in range(2):
        wcopy(jnp.int32(0), m).start()
    for cp in second:
        cp.wait()
    for j in range(1, C):
        sums1(j)
        for k in range(3):
            ss1copy(j, k).start()
    xcopy(1).start()

    @pl.loop(TP, 2 * TP)
    def _(t):
        for m in range(2):
            wcopy(t, m).start()

    for b in range(2):
        for t in range(QT):
            wqcopy(b, t).start()

    def norm1(j):
        if j == 0:
            rwait(ss1.at[0, pl.ds(0, 3)], ss1_r.at[0])
        elif j == 1:
            rwait(ss1.at[pl.ds(1, C - 1), pl.ds(0, 3)], ss1_r.at[1])
        rr = row_scales(ss1.at[j])
        rows = pl.ds(j * T, T)
        for half in range(2):
            for l in range(HL // 128):
                cols = pl.ds(half * HL + l * 128, 128)
                xb = xv[rows, pl.ds(l * 128, 128)] if half == 0 else nf2[rows, cols]
                nf[rows, cols] = (xb.astype(F32) * rr * g1v[:, cols]).astype(BF16)

    gcp.wait_recv()
    xcopy(0).wait_recv()
    norm1(0)

    def pcopy(j, t):
        s2 = lax.rem(j, 2)
        s3 = lax.rem(j, 3)
        return rcopy(psnd.at[s2, t], prcv.at[s3, t], p_s.at[s2], p_r.at[s3], XP)

    def gu(g, row, n):
        bs = lax.rem(g, NB)
        nn = nf[pl.ds(row, n), :]
        return _dot(nn, wbuf[bs, 0]), _dot(nn, wbuf[bs, 1])

    def prefetch(g):
        @pl.when(g < NL)
        def _():
            start_own(g)
            start_sib(g)

    def put_send(j, t, gg, uu):
        s2 = lax.rem(j, 2)
        psnd[s2, t, :, 0:NT] = gg
        psnd[s2, t, :, NT:2 * NT] = uu
        pcopy(j, t).start()

    def s12(j):
        s2 = lax.rem(j, 2)
        g0 = 3 * TP + (j - 2) * (2 * TP)
        rwait(psnd.at[s2], p_s.at[s2])
        row = mo(j * T, T)

        @pl.loop(0, TP)
        def _(t):
            wait_tile(g0 + t)
            prefetch(g0 + t + NB - 1)
            gg, uu = gu(g0 + t, row, T)
            put_send(j, t, gg, uu)

        @pl.loop(0, TP)
        def _(t):
            wait_tile(g0 + t + TP)
            prefetch(g0 + t + TP + NB - 1)
            gg, uu = gu(g0 + t + TP, row, T)
            pkeep[s2, t, :, 0:NT] = gg
            pkeep[s2, t, :, NT:2 * NT] = uu

    def acopy(i, k):
        sl = lax.rem(i, 3)
        b = (h, h, hx)[k]
        return rcopy(abuf.at[sl, b], abuf.at[sl, b], a_s.at[sl], a_r.at[sl, k], (XP, SIB, SIB)[k])

    def s3(i):
        s2 = lax.rem(i, 2)
        sl = lax.rem(i, 3)

        rwait(prcv.at[sl], p_r.at[sl])

        @pl.loop(0, TP)
        def _(t):
            gg = pkeep[s2, t, :, 0:NT] + prcv[sl, t, :, 0:NT]
            uu = pkeep[s2, t, :, NT:2 * NT] + prcv[sl, t, :, NT:2 * NT]
            abuf[sl, h, :, pl.ds(mo(t * NT, NT), NT)] = (gg * jax.nn.sigmoid(gg) * uu).astype(BF16)

        acopy(i, 0).start()
        acopy(i, 1).start()

    def ycopy(i, n):
        s2 = lax.rem(i, 2)
        cols = pl.ds(mo(n * NT, NT), NT)
        sl = lax.rem(i, 3)
        return rcopy(ysnd.at[s2, :, cols], yrcv.at[sl, :, cols], y_s.at[s2], y_r.at[sl], YP)

    def down(sl, b, n):
        return _dot(abuf[sl, b], wd[n, pl.ds(mo(b * FB, FB), FB)])

    def s4a(i):
        s2 = lax.rem(i, 2)
        sl = lax.rem(i, 3)
        acopy(i, 1).wait_recv()

        @pl.loop(0, DT)
        def _(n):
            acc = _dot(ov[pl.ds(mo(i * T, T), T), :], wo[n])
            acc += down(sl, h, n)
            acc += down(sl, hs, n)
            ysnd[s2, :, pl.ds(mo(n * NT, NT), NT)] = acc

    def s4b(i):
        s2 = lax.rem(i, 2)
        sl = lax.rem(i, 3)
        acopy(i, 0).wait_recv()
        acopy(i, 2).start()
        acopy(i, 2).wait_recv()

        @pl.loop(0, DT)
        def _(n):
            ysnd[s2, :, pl.ds(mo(n * NT, NT), NT)] += down(sl, hx, n) + down(sl, hd, n)
            ycopy(i, n).start()

    def ss2copy(i, k):
        dev = (XP, SIB, DIAG)[k]
        return rcopy(ss2.at[i, h], ss2.at[i, h], ss2_s, ss2_r.at[lax.rem(i, 4)], dev)

    def s5(i):
        s2 = lax.rem(i, 2)
        sl = lax.rem(i, 3)
        rwait(abuf.at[sl, pl.ds(0, 3)], a_s.at[sl])
        rwait(ysnd.at[s2], y_s.at[s2])
        rwait(yrcv.at[sl], y_r.at[sl])
        rows = pl.ds(mo(i * T, T), T)
        xn = (xv[rows, :].astype(F32) + (ysnd[s2] + yrcv[sl])).astype(BF16)
        xov[rows, :] = xn
        ss2[i, h] = row_sums(xn.astype(F32))
        for k in range(3):
            ss2copy(i, k).start()

    def n2copy(i):
        rows = pl.ds(mo(i * T, T), T)
        return rcopy(nf2.at[rows, pl.ds(0, HL)], nf2.at[rows, pl.ds(HL, HL)], n2_s, n2_r.at[i], SIB)

    def s6(i):
        rows = pl.ds(mo(i * T, T), T)
        rwait(ss2.at[i, pl.ds(0, 3)], ss2_r.at[lax.rem(i, 4)])
        rr = row_scales(ss2.at[i])
        for l in range(HL // 128):
            xf = xov[rows, pl.ds(l * 128, 128)].astype(F32)
            nf2[rows, pl.ds(l * 128, 128)] = (xf * rr * g2v[:, pl.ds(l * 128, 128)]).astype(BF16)
        n2copy(i).start()

    def qcopy(i):
        return rcopy(qsnd.at[i], qrcv.at[i], q_s, q_r.at[i], XP)

    def s7(i):
        n2copy(i).wait_recv()
        nn = nf2[pl.ds(mo(i * T, T), T), :]
        for t in range(QT):
            qsnd[i, :, t * NT:(t + 1) * NT] = _dot(nn, wq[0, t])
        qcopy(i).start()
        for t in range(QT):
            qkeep[i, :, t * NT:(t + 1) * NT] = _dot(nn, wq[1, t])

    def qacopy(i, k):
        b = (h, h, hx)[k]
        dev = (XP, SIB, SIB)[k]
        blk = qall.at[pl.ds(mo(i * T, T), T), pl.ds(mo(b * QB, NT), QB)]
        return rcopy(blk, blk, qa_s, qa_r.at[i if k == 0 else C], dev)

    def s8(i, late=False):
        qcopy(i).wait_recv()
        for t in range(QT):
            cols = pl.ds(t * NT, NT)
            qall[pl.ds(mo(i * T, T), T), pl.ds(mo(h * QB + t * NT, NT), NT)] = (qkeep[i, :, cols] + qrcv[i, :, cols]).astype(BF16)
        qacopy(i, 1).start()
        if late:
            pl.when(c == 0)(qacopy(i, 0).start)
        else:
            qacopy(i, 0).start()

    def s9a(i):
        qacopy(i, 0).wait_recv()
        qacopy(i, 2).start()

    lwait(wbuf.at[0, :, pl.ds(0, HL)], ld_sem.at[0])
    for m in range(2):
        cols = pl.ds(m * NT, NT)
        rwait(wbuf.at[0, m, pl.ds(HL, HL)], w0_r.at[m])
        psnd[0, 0, :, cols] = _dot(nf[top, :], wbuf[0, m])
        rcopy(psnd.at[0, 0, :, cols], prcv.at[0, 0, :, cols], p_s.at[0], p_r.at[0], XP).start()
    start_own(jnp.int32(2))
    start_sib(jnp.int32(1))

    @pl.loop(1, TP)
    def _(t):
        wait_tile(t)
        gg, uu = gu(t, 0, T)
        put_send(jnp.int32(0), t, gg, uu)
        start_own(t + 2)
        start_sib(t + 1)

    start_sib(jnp.int32(TP + 1))
    for g in range(TP + 2, TP + NB - 1):
        prefetch(jnp.int32(g))
    xcopy(1).wait_recv()
    for j in range(1, C):
        norm1(j)

    @pl.loop(0, TP)
    def _(t):
        wait_tile(TP + t)
        prefetch(TP + t + NB - 1)
        gg, uu = gu(TP + t, T, T)
        put_send(jnp.int32(1), t, gg, uu)


    res = [[] for _ in range(4)]
    for n in range(DT):
        res[n % 4].append(lcopy(wd_hbm.at[:, pl.ds(n * NT, NT)], wd.at[n], in_sem.at[1]))
        res[n % 4].append(lcopy(wo_hbm.at[:, pl.ds(n * NT, NT)], wo.at[n], in_sem.at[2]))
    res[0].append(lcopy(o_hbm, ov, in_sem.at[0]))
    for b in range(2):
        blk = (hx, h)[b]
        for t in range(QT):
            res[3].append(lcopy(wq_hbm.at[:, pl.ds(mo(blk * QB + t * NT, NT), NT)], wq.at[b, t, pl.ds(0, HL)],
                                in_sem.at[3]))

    @pl.loop(0, TP)
    def _(t):
        wait_tile(2 * TP + t)
        prefetch(2 * TP + t + NB - 1)
        for k in range(4):
            @pl.when(t == k)
            def _(k=k):
                for cp in res[k]:
                    cp.start()

        gg, uu = gu(2 * TP + t, 0, 2 * T)
        for j in range(2):
            pkeep[j, t, :, 0:NT] = gg[j * T:(j + 1) * T]
            pkeep[j, t, :, NT:2 * NT] = uu[j * T:(j + 1) * T]

    def stage(fn, i, lo=0):
        @pl.when((i >= lo) & (i < C))
        def _():
            fn(i)

    def loaded():
        lwait(ov, in_sem.at[0])
        lwait(wd, in_sem.at[1])
        lwait(wo, in_sem.at[2])
        lwait(wq.at[:, :, pl.ds(0, HL)], in_sem.at[3])
        rwait(wq.at[:, :, pl.ds(HL, HL)], wq_s)
        rwait(wq.at[:, :, pl.ds(HL, HL)], wq_r)

    @pl.loop(0, C - 2)
    def _(i):
        s3(i)
        s12(i + 2)

        @pl.when(i == 0)
        def _():
            loaded()

        stage(s5, i - 1)
        s4a(i)
        s4b(i)
        stage(s6, i - 2)

    e = C - 1
    done = {s7: 0, s8: 0, s9a: 0}

    def run(*steps):
        for fn, i in steps:
            fn(jnp.int32(i))

    def nxt(*fns):
        for fn in fns:
            if done[fn] < C:
                fn(jnp.int32(done[fn]))
                done[fn] += 1

    run((s3, e - 1), (s4a, e - 1), (s5, e - 2), (s6, e - 3), (s3, e))
    nxt(s7)
    run((s4b, e - 1))
    nxt(s7)
    run((s4a, e), (s6, e - 2), (s4b, e))
    nxt(s7, s8)
    run((s5, e - 1))
    nxt(s7, s8)
    run((s5, e), (s6, e - 1))
    nxt(s7, s8)
    run((s6, e))
    nxt(s7, s8, s9a, s7, s8, s9a, s7, s9a)
    gcp.wait_send()
    rwait(ss1.at[:, pl.ds(0, 3)], ss1_s)
    for k in range(2):
        xcopy(k).wait_send()

    rwait(wsib_hbm, ws_s)
    rwait(wbuf.at[0, :, pl.ds(HL, HL)], w0_s)

    for k in range(2):
        rwait(psnd.at[k], p_s.at[k])

    while done[s8] < C - HOLD - 1:
        nxt(s8, s9a)
    while done[s8] < C - 1:
        s8(jnp.int32(done[s8]), late=True)
        done[s8] += 1
        if done[s9a] < C - HOLD - 1:
            nxt(s9a)

    s8(jnp.int32(C - 1), late=True)

    @pl.when(c == 1)
    def _():
        for i in range(C - HOLD - 1, C):
            qacopy(jnp.int32(i), 0).start()

    rwait(ss2.at[:, pl.ds(0, 3)], ss2_s)
    rwait(nf2.at[:, pl.ds(0, HL)], n2_s)
    rwait(qsnd, q_s)

    while done[s9a] < C:
        nxt(s9a)
    rwait(qall.at[:, pl.ds(0, 2 * QB)], qa_r.at[C])
    rwait(qall.at[:, pl.ds(0, 3 * QB)], qa_s)


def _out_kernel(xv, qv, xo, qo, sem):
    n = xv.shape[0] // 4
    cps = [pltpu.make_async_copy(a.at[pl.ds(k * n, n)], b.at[pl.ds(k * n, n)], sem.at[m, k])
           for m, (a, b) in enumerate(((qv, qo), (xv, xo))) for k in range(4)]
    for cp in cps:
        cp.start()
    for cp in cps:
        cp.wait()


def solution(mesh):
    nh = mesh.shape['h']

    def body(x, g1, g2, w_gate, w_up, w_down, o, w_o, w_qkv):
        S, HL = x.shape
        FL = w_gate.shape[1]
        FB = FL // nh
        QL = w_qkv.shape[1]
        QB = QL // nh
        OL = o.shape[1]
        T = 64
        C = S // T
        TP, QT, DT = FB // NT, QB // NT, HL // NT
        d = HL * nh
        any_ = pl.BlockSpec(memory_space=pl.ANY)
        vm = pl.BlockSpec(memory_space=pltpu.VMEM)
        dma = pltpu.SemaphoreType.DMA
        V = pltpu.VMEM
        scratch = [
            V((S, HL), BF16), V((1, 2 * HL), F32), V((1, HL), F32), V((S, OL), BF16),
            V((DT, FL, NT), BF16), V((DT, OL, NT), BF16), V((2, QT, 2 * HL, NT), BF16),
            V((NB, 2, 2 * HL, NT), BF16), V((S, 2 * HL), BF16), V((C, nh, 1, 128), F32),
            V((2, TP, T, 2 * NT), F32), V((3, TP, T, 2 * NT), F32), V((2, TP, T, 2 * NT), F32),
            V((3, nh, T, FB), BF16), V((2, T, HL), F32), V((3, T, HL), F32),
            V((C, nh, 1, 128), F32), V((S, 2 * HL), BF16),
            V((C, T, QB), F32), V((C, T, QB), F32), V((C, T, QB), F32),
            dma((4,)), dma((NB,)), dma, dma((2,)), dma, dma((2 * TP,)), dma, dma,
            dma((3,)), dma((3,)), dma, dma((2,)), dma((2,)), dma((3,)), dma((3,)), dma((3, 3)), dma((2,)), dma((3,)),
            dma, dma((4,)), dma, dma((C,)), dma, dma((C,)), dma, dma((C + 1,)),
        ]
        xo, qo, _ = pl.pallas_call(
            functools.partial(_kernel, T, C, float(d)),
            out_shape=(V((S, HL), BF16), V((S, QL), BF16), jax.ShapeDtypeStruct((2 * TP, 2, HL, NT), BF16)),
            in_specs=[any_] * 9,
            out_specs=(vm, vm, any_),
            scratch_shapes=scratch,
            compiler_params=pltpu.CompilerParams(collective_id=0, has_side_effects=True, vmem_limit_bytes=56 * 2**20),
            name='block',
        )(x, g1.reshape(1, HL), g2.reshape(1, HL), w_gate, w_up, w_down, o, w_o, w_qkv)
        return pl.pallas_call(
            _out_kernel,
            out_shape=(jax.ShapeDtypeStruct((S, HL), BF16), jax.ShapeDtypeStruct((S, QL), BF16)),
            in_specs=[vm, vm],
            out_specs=(any_, any_),
            scratch_shapes=[dma((2, 4))],
            compiler_params=pltpu.CompilerParams(vmem_limit_bytes=2**20),
            name='out',
        )(xo, qo)

    in_specs = (P(None, 'h'), P('h'), P('h'), P('h', 'f'), P('h', 'f'), P('f', 'h'),
                P(None, 'f'), P('f', 'h'), P('h', 'f'))
    return jax.shard_map(body, mesh=mesh, in_specs=in_specs,
                         out_specs=(P(None, 'h'), P(None, 'f')), check_vma=False)
```

```python
import functools

import jax
import jax.numpy as jnp
from jax import lax
from jax.experimental import pallas as pl
from jax.experimental.pallas import tpu as pltpu
from jax.sharding import PartitionSpec as P

EPS = 1e-6
MESH = pl.DeviceIdType.MESH
F32 = jnp.float32
BF16 = jnp.bfloat16
NT = 256
NB = 4
HOLD = 2
DIRECT = 16


def _dot(a, b):
    return jnp.dot(a, b, preferred_element_type=F32)


def _kernel(T, C, d,
            x_hbm, g1_hbm, g2_hbm, wg_hbm, wu_hbm, wd_hbm, o_hbm, wo_hbm, wq_hbm,
            xov, qall, wsib_hbm,
            xv, g1v, g2v, ov, wd, wo, wq, wbuf, nf, ss1, psnd, prcv, pkeep, abuf, ysnd, yrcv, ss2, nf2,
            qsnd, qrcv, qkeep,
            in_sem, ld_sem, w0_s, ws_s, wq_s, ss1_s, p_s, p_r, a_s, a_r, y_s, y_r, ss2_s, ss2_r, n2_s, q_s, qa_s,
            pool_a, pool_b):
    ws_r, n2_r, q_r = pool_a, pool_a.at[pl.ds(0, C)], pool_a.at[pl.ds(C, C)]
    n_s, n_r, w0_r, ss1_r, wq_r = (pool_b.at[pl.ds(0, 3)], pool_b.at[pl.ds(3, 3)], pool_b.at[pl.ds(6, 2)],
                                   pool_b.at[pl.ds(8, 2)], pool_b.at[10])
    qa_r = pool_b
    S = xv.shape[0]
    HL = xv.shape[1]
    FB = abuf.shape[3]
    QB = qsnd.shape[2]
    TP = FB // NT
    QT = QB // NT
    DT = HL // NT
    f = lax.axis_index('f')
    h = lax.axis_index('h')
    c = lax.rem(h, 2)
    xx = h // 2
    hx = (1 - xx) * 2 + c
    hs = xx * 2 + (1 - c)
    hd = (1 - xx) * 2 + (1 - c)
    XP, SIB, DIAG, YP = (f, hx), (f, hs), (f, hd), (1 - f, h)

    def rcopy(src, dst, s, r, dev):
        return pltpu.make_async_remote_copy(src_ref=src, dst_ref=dst, send_sem=s, recv_sem=r, device_id=dev,
                                            device_id_type=MESH)

    def lcopy(src, dst, s):
        return pltpu.make_async_copy(src, dst, s)

    def lwait(ref, sem):
        lcopy(ref, ref, sem).wait()

    def rwait(ref, sem):
        rcopy(ref, ref, sem, sem, XP).wait_recv()

    def mo(v, m):
        return pl.multiple_of(v, m)

    top, rest = pl.ds(0, T), pl.ds(T, S - T)
    first = [lcopy(x_hbm.at[top], xv.at[top], in_sem.at[0]), lcopy(g1_hbm, g1v.at[:, pl.ds(0, HL)], in_sem.at[1])]
    second = [lcopy(x_hbm.at[rest], xv.at[rest], in_sem.at[2]), lcopy(g2_hbm, g2v, in_sem.at[3])]
    for cp in first:
        cp.start()

    bar = pltpu.get_barrier_semaphore()
    for dev in (XP, SIB, DIAG, YP):
        pl.semaphore_signal(bar, inc=1, device_id=dev, device_id_type=MESH)

    NL = 3 * TP + (C - 2) * 2 * TP

    def tile_of(g):
        return jnp.where(g < TP, g, lax.rem(g + TP, 2 * TP))

    def own(g):
        t = tile_of(g)
        bs = lax.rem(g, NB)
        blk = jnp.where(t < TP, hx, h)
        col = mo(blk * FB + lax.rem(t, TP) * NT, NT)
        return (lcopy(wg_hbm.at[:, pl.ds(col, NT)], wbuf.at[bs, 0, pl.ds(0, HL)], ld_sem.at[bs]),
                lcopy(wu_hbm.at[:, pl.ds(col, NT)], wbuf.at[bs, 1, pl.ds(0, HL)], ld_sem.at[bs]))

    def sib(g):
        t = tile_of(g)
        bs = lax.rem(g, NB)
        return (lcopy(wsib_hbm.at[t, 0], wbuf.at[bs, 0, pl.ds(HL, HL)], ld_sem.at[bs]),
                lcopy(wsib_hbm.at[t, 1], wbuf.at[bs, 1, pl.ds(HL, HL)], ld_sem.at[bs]))

    def wcopy(t, m):
        blk = jnp.where(t < TP, hd, hs)
        col = mo(blk * FB + lax.rem(t, TP) * NT, NT)
        src = (wg_hbm, wu_hbm)[m].at[:, pl.ds(col, NT)]
        return rcopy(src, wsib_hbm.at[t, m], ws_s, ws_r.at[t], SIB)

    def wqcopy(b, t):
        blk = (hd, hs)[b]
        col = mo(blk * QB + t * NT, NT)
        return rcopy(wq_hbm.at[:, pl.ds(col, NT)], wq.at[b, t, pl.ds(HL, HL)], wq_s, wq_r, SIB)

    def start_sib(g):
        @pl.when((g <= TP) | ((g >= 2 * TP) & (g < 3 * TP)))
        def _():
            t = tile_of(g)
            rwait(wsib_hbm.at[t], ws_r.at[t])

        for cp in sib(g):
            cp.start()

    def start_own(g):
        for cp in own(g):
            cp.start()

    def wait_tile(g):
        bs = lax.rem(g, NB)
        lwait(wbuf.at[bs], ld_sem.at[bs])

    first[0].wait()
    start_own(jnp.int32(0))
    for cp in second:
        cp.start()
    start_own(jnp.int32(1))

    def row_sums(xf):
        s = jnp.broadcast_to(jnp.sum(xf * xf, axis=1, keepdims=True), (T, 128))
        if T < 128:
            s = jnp.concatenate([s] * (128 // T), axis=0)
        return s.T[0:1]

    def row_scales(ss):
        r = lax.rsqrt((ss[0] + ss[1] + ss[2] + ss[3]) / d + EPS)
        return jnp.broadcast_to(r, (128, 128)).T[0:T]

    def sums1(j):
        ss1[j, h] = row_sums(xv[pl.ds(j * T, T), :].astype(F32))

    sums1(0)

    def ss1copy(j, k):
        dev = (XP, SIB, DIAG)[k]
        return rcopy(ss1.at[j, h], ss1.at[j, h], ss1_s, ss1_r.at[min(j, 1)], dev)

    def xcopy(k):
        rows = (top, rest)[k]
        return rcopy(xv.at[rows], nf2.at[rows, pl.ds(HL, HL)], n_s.at[k], n_r.at[k], SIB)

    gcp = rcopy(g1v.at[:, pl.ds(0, HL)], g1v.at[:, pl.ds(HL, HL)], n_s.at[2], n_r.at[2], SIB)

    first[1].wait()
    pl.semaphore_wait(bar, 4)
    for k in (0, 2, 1):
        ss1copy(0, k).start()
    xcopy(0).start()
    gcp.start()
    def w0copy(m):
        src = (wg_hbm, wu_hbm)[m].at[:, pl.ds(mo(hd * FB, NT), NT)]
        return rcopy(src, wbuf.at[0, m, pl.ds(HL, HL)], w0_s, w0_r.at[m], SIB)

    for m in range(2):
        w0copy(m).start()

    @pl.loop(1, TP)
    def _(t):
        for m in range(2):
            wcopy(t, m).start()

    for m in range(2):
        wcopy(jnp.int32(0), m).start()
    for cp in second:
        cp.wait()
    for j in range(1, C):
        sums1(j)
        for k in range(3):
            ss1copy(j, k).start()
    xcopy(1).start()

    @pl.loop(TP, 2 * TP)
    def _(t):
        for m in range(2):
            wcopy(t, m).start()

    for b in range(2):
        for t in range(QT):
            wqcopy(b, t).start()

    def norm1(j):
        if j == 0:
            rwait(ss1.at[0, pl.ds(0, 3)], ss1_r.at[0])
        elif j == 1:
            rwait(ss1.at[pl.ds(1, C - 1), pl.ds(0, 3)], ss1_r.at[1])
        rr = row_scales(ss1.at[j])
        rows = pl.ds(j * T, T)
        for half in range(2):
            for l in range(HL // 128):
                cols = pl.ds(half * HL + l * 128, 128)
                xb = xv[rows, pl.ds(l * 128, 128)] if half == 0 else nf2[rows, cols]
                nf[rows, cols] = (xb.astype(F32) * rr * g1v[:, cols]).astype(BF16)

    gcp.wait_recv()
    xcopy(0).wait_recv()
    norm1(0)

    def pcopy(j, t):
        s2 = lax.rem(j, 2)
        s3 = lax.rem(j, 3)
        return rcopy(psnd.at[s2, t], prcv.at[s3, t], p_s.at[s2], p_r.at[s3], XP)

    def gu(g, row, n):
        bs = lax.rem(g, NB)
        nn = nf[pl.ds(row, n), :]
        return _dot(nn, wbuf[bs, 0]), _dot(nn, wbuf[bs, 1])

    def prefetch(g):
        @pl.when(g < NL)
        def _():
            start_own(g)
            start_sib(g)

    def put_send(j, t, gg, uu):
        s2 = lax.rem(j, 2)
        psnd[s2, t, :, 0:NT] = gg
        psnd[s2, t, :, NT:2 * NT] = uu
        pcopy(j, t).start()

    def s12(j):
        s2 = lax.rem(j, 2)
        g0 = 3 * TP + (j - 2) * (2 * TP)
        rwait(psnd.at[s2], p_s.at[s2])
        row = mo(j * T, T)

        @pl.loop(0, TP)
        def _(t):
            wait_tile(g0 + t)
            prefetch(g0 + t + NB - 1)
            gg, uu = gu(g0 + t, row, T)
            put_send(j, t, gg, uu)

        @pl.loop(0, TP)
        def _(t):
            wait_tile(g0 + t + TP)
            prefetch(g0 + t + TP + NB - 1)
            gg, uu = gu(g0 + t + TP, row, T)
            pkeep[s2, t, :, 0:NT] = gg
            pkeep[s2, t, :, NT:2 * NT] = uu

    def acopy(i, k):
        sl = lax.rem(i, 3)
        b = (h, h, hx)[k]
        return rcopy(abuf.at[sl, b], abuf.at[sl, b], a_s.at[sl], a_r.at[sl, k], (XP, SIB, SIB)[k])

    def s3(i):
        s2 = lax.rem(i, 2)
        sl = lax.rem(i, 3)

        rwait(prcv.at[sl], p_r.at[sl])

        @pl.loop(0, TP)
        def _(t):
            gg = pkeep[s2, t, :, 0:NT] + prcv[sl, t, :, 0:NT]
            uu = pkeep[s2, t, :, NT:2 * NT] + prcv[sl, t, :, NT:2 * NT]
            abuf[sl, h, :, pl.ds(mo(t * NT, NT), NT)] = (gg * jax.nn.sigmoid(gg) * uu).astype(BF16)

        acopy(i, 0).start()
        acopy(i, 1).start()

    def ycopy(i, n):
        s2 = lax.rem(i, 2)
        cols = pl.ds(mo(n * NT, NT), NT)
        sl = lax.rem(i, 3)
        return rcopy(ysnd.at[s2, :, cols], yrcv.at[sl, :, cols], y_s.at[s2], y_r.at[sl], YP)

    def down(sl, b, n):
        return _dot(abuf[sl, b], wd[n, pl.ds(mo(b * FB, FB), FB)])

    def s4a(i):
        s2 = lax.rem(i, 2)
        sl = lax.rem(i, 3)
        acopy(i, 1).wait_recv()

        @pl.loop(0, DT)
        def _(n):
            acc = _dot(ov[pl.ds(mo(i * T, T), T), :], wo[n])
            acc += down(sl, h, n)
            acc += down(sl, hs, n)
            ysnd[s2, :, pl.ds(mo(n * NT, NT), NT)] = acc

    def s4b(i):
        s2 = lax.rem(i, 2)
        sl = lax.rem(i, 3)
        acopy(i, 0).wait_recv()
        acopy(i, 2).start()
        acopy(i, 2).wait_recv()

        @pl.loop(0, DT)
        def _(n):
            ysnd[s2, :, pl.ds(mo(n * NT, NT), NT)] += down(sl, hx, n) + down(sl, hd, n)
            ycopy(i, n).start()

    def ss2copy(i, k):
        dev = (XP, SIB, DIAG)[k]
        return rcopy(ss2.at[i, h], ss2.at[i, h], ss2_s, ss2_r.at[lax.rem(i, 4)], dev)

    def s5(i):
        s2 = lax.rem(i, 2)
        sl = lax.rem(i, 3)
        rwait(abuf.at[sl, pl.ds(0, 3)], a_s.at[sl])
        rwait(ysnd.at[s2], y_s.at[s2])
        rwait(yrcv.at[sl], y_r.at[sl])
        rows = pl.ds(mo(i * T, T), T)
        xn = (xv[rows, :].astype(F32) + (ysnd[s2] + yrcv[sl])).astype(BF16)
        xov[rows, :] = xn
        ss2[i, h] = row_sums(xn.astype(F32))
        for k in range(3):
            ss2copy(i, k).start()

    def n2copy(i):
        rows = pl.ds(mo(i * T, T), T)
        return rcopy(nf2.at[rows, pl.ds(0, HL)], nf2.at[rows, pl.ds(HL, HL)], n2_s, n2_r.at[i], SIB)

    def s6(i):
        rows = pl.ds(mo(i * T, T), T)
        rwait(ss2.at[i, pl.ds(0, 3)], ss2_r.at[lax.rem(i, 4)])
        rr = row_scales(ss2.at[i])
        for l in range(HL // 128):
            xf = xov[rows, pl.ds(l * 128, 128)].astype(F32)
            nf2[rows, pl.ds(l * 128, 128)] = (xf * rr * g2v[:, pl.ds(l * 128, 128)]).astype(BF16)
        n2copy(i).start()

    def qcopy(i):
        return rcopy(qsnd.at[i], qrcv.at[i], q_s, q_r.at[i], XP)

    def s7(i):
        n2copy(i).wait_recv()
        nn = nf2[pl.ds(mo(i * T, T), T), :]
        for t in range(QT):
            qsnd[i, :, t * NT:(t + 1) * NT] = _dot(nn, wq[0, t])
        qcopy(i).start()
        for t in range(QT):
            qkeep[i, :, t * NT:(t + 1) * NT] = _dot(nn, wq[1, t])

    def qacopy(i, k, last=False):
        b = (h, h, hx)[k]
        dev = (XP, SIB, SIB)[k]
        n = T - DIRECT if last and k != 1 else T
        blk = qall.at[pl.ds(mo(i * T, T), n), pl.ds(mo(b * QB, NT), QB)]
        return rcopy(blk, blk, qa_s, qa_r.at[(i, C, C + 2)[k]], dev)

    def direct(k):
        blk = qall.at[pl.ds(S - DIRECT, DIRECT), pl.ds(mo(h * QB, NT), QB)]
        return rcopy(blk, blk, qa_s, qa_r.at[C + 1], (XP, DIAG)[k])

    def s8(i, late=False):
        qcopy(i).wait_recv()
        for t in range(QT):
            cols = pl.ds(t * NT, NT)
            qall[pl.ds(mo(i * T, T), T), pl.ds(mo(h * QB + t * NT, NT), NT)] = (qkeep[i, :, cols] + qrcv[i, :, cols]).astype(BF16)
        qacopy(i, 1).start()
        if late:
            pl.when(c == 0)(qacopy(i, 0).start)
        else:
            qacopy(i, 0).start()

    def s9a(i):
        qacopy(i, 0).wait_recv()
        qacopy(i, 2).start()

    lwait(wbuf.at[0, :, pl.ds(0, HL)], ld_sem.at[0])
    for m in range(2):
        cols = pl.ds(m * NT, NT)
        rwait(wbuf.at[0, m, pl.ds(HL, HL)], w0_r.at[m])
        psnd[0, 0, :, cols] = _dot(nf[top, :], wbuf[0, m])
        rcopy(psnd.at[0, 0, :, cols], prcv.at[0, 0, :, cols], p_s.at[0], p_r.at[0], XP).start()
    start_own(jnp.int32(2))
    start_sib(jnp.int32(1))

    @pl.loop(1, TP)
    def _(t):
        wait_tile(t)
        gg, uu = gu(t, 0, T)
        put_send(jnp.int32(0), t, gg, uu)
        start_own(t + 2)
        start_sib(t + 1)

    start_sib(jnp.int32(TP + 1))
    for g in range(TP + 2, TP + NB - 1):
        prefetch(jnp.int32(g))
    xcopy(1).wait_recv()
    for j in range(1, C):
        norm1(j)

    @pl.loop(0, TP)
    def _(t):
        wait_tile(TP + t)
        prefetch(TP + t + NB - 1)
        gg, uu = gu(TP + t, T, T)
        put_send(jnp.int32(1), t, gg, uu)


    res = [[] for _ in range(4)]
    for n in range(DT):
        res[n % 4].append(lcopy(wd_hbm.at[:, pl.ds(n * NT, NT)], wd.at[n], in_sem.at[1]))
        res[n % 4].append(lcopy(wo_hbm.at[:, pl.ds(n * NT, NT)], wo.at[n], in_sem.at[2]))
    res[0].append(lcopy(o_hbm, ov, in_sem.at[0]))
    for b in range(2):
        blk = (hx, h)[b]
        for t in range(QT):
            res[3].append(lcopy(wq_hbm.at[:, pl.ds(mo(blk * QB + t * NT, NT), NT)], wq.at[b, t, pl.ds(0, HL)],
                                in_sem.at[3]))

    @pl.loop(0, TP)
    def _(t):
        wait_tile(2 * TP + t)
        prefetch(2 * TP + t + NB - 1)
        for k in range(4):
            @pl.when(t == k)
            def _(k=k):
                for cp in res[k]:
                    cp.start()

        gg, uu = gu(2 * TP + t, 0, 2 * T)
        for j in range(2):
            pkeep[j, t, :, 0:NT] = gg[j * T:(j + 1) * T]
            pkeep[j, t, :, NT:2 * NT] = uu[j * T:(j + 1) * T]

    gcp.wait_send()
    rwait(ss1.at[:, pl.ds(0, 3)], ss1_s)
    for k in range(2):
        xcopy(k).wait_send()

    def stage(fn, i, lo=0):
        @pl.when((i >= lo) & (i < C))
        def _():
            fn(i)

    def loaded():
        lwait(ov, in_sem.at[0])
        lwait(wd, in_sem.at[1])
        lwait(wo, in_sem.at[2])
        lwait(wq.at[:, :, pl.ds(0, HL)], in_sem.at[3])
        rwait(wq.at[:, :, pl.ds(HL, HL)], wq_s)
        rwait(wq.at[:, :, pl.ds(HL, HL)], wq_r)

    @pl.loop(0, C - 2)
    def _(i):
        s3(i)
        s12(i + 2)

        @pl.when(i == 0)
        def _():
            loaded()

        stage(s5, i - 1)
        s4a(i)
        s4b(i)
        stage(s6, i - 2)

    e = C - 1
    done = {s7: 0, s8: 0, s9a: 0}

    def run(*steps):
        for fn, i in steps:
            fn(jnp.int32(i))

    def nxt(*fns):
        for fn in fns:
            if done[fn] < C:
                fn(jnp.int32(done[fn]))
                done[fn] += 1

    run((s3, e - 1), (s4a, e - 1), (s5, e - 2), (s6, e - 3), (s3, e))
    nxt(s7)
    run((s4b, e - 1))
    nxt(s7)
    run((s4a, e), (s6, e - 2), (s4b, e))
    nxt(s7, s8)
    run((s5, e - 1))
    nxt(s7, s8)
    run((s5, e), (s6, e - 1))
    nxt(s7, s8)
    run((s6, e))
    nxt(s7, s8, s9a, s7, s8, s9a, s7, s9a)
    rwait(wsib_hbm, ws_s)
    rwait(wbuf.at[0, :, pl.ds(HL, HL)], w0_s)

    for k in range(2):
        rwait(psnd.at[k], p_s.at[k])

    while done[s8] < C - HOLD - 1:
        nxt(s8, s9a)
    while done[s8] < C - 1:
        s8(jnp.int32(done[s8]), late=True)
        done[s8] += 1
        if done[s9a] < C - HOLD - 1:
            nxt(s9a)

    s8(jnp.int32(C - 1), late=True)

    @pl.when(c == 1)
    def _():
        for i in range(C - HOLD - 1, C - 1):
            qacopy(jnp.int32(i), 0).start()
        qacopy(jnp.int32(C - 1), 0, last=True).start()
        direct(0).start()
        direct(1).start()

    rwait(ss2.at[:, pl.ds(0, 3)], ss2_s)
    rwait(nf2.at[:, pl.ds(0, HL)], n2_s)
    rwait(qsnd, q_s)

    while done[s9a] < C - 1:
        nxt(s9a)
    e = jnp.int32(C - 1)
    rows = pl.ds(0, DIRECT)

    @pl.when(c == 0)
    def _():
        s9a(e)
        rwait(qall.at[pl.ds(0, S - DIRECT), pl.ds(0, QB)], qa_r.at[C + 2])
        rwait(qall.at[rows, pl.ds(0, QB)], qa_r.at[C + 1])

    @pl.when(c == 1)
    def _():
        qacopy(e, 0, last=True).wait_recv()
        qacopy(e, 2, last=True).start()
        rwait(qall.at[:, pl.ds(0, QB)], qa_r.at[C + 2])
        rwait(qall.at[rows, pl.ds(0, QB)], qa_r.at[C + 1])

    rwait(qall.at[:, pl.ds(0, QB)], qa_r.at[C])
    rwait(qall.at[:, pl.ds(0, 3 * QB)], qa_s)


def _out_kernel(xv, qv, xo, qo, sem):
    n = xv.shape[0] // 4
    cps = [pltpu.make_async_copy(a.at[pl.ds(k * n, n)], b.at[pl.ds(k * n, n)], sem.at[m, k])
           for m, (a, b) in enumerate(((qv, qo), (xv, xo))) for k in range(4)]
    for cp in cps:
        cp.start()
    for cp in cps:
        cp.wait()


def solution(mesh):
    nh = mesh.shape['h']

    def body(x, g1, g2, w_gate, w_up, w_down, o, w_o, w_qkv):
        S, HL = x.shape
        FL = w_gate.shape[1]
        FB = FL // nh
        QL = w_qkv.shape[1]
        QB = QL // nh
        OL = o.shape[1]
        T = 64
        C = S // T
        TP, QT, DT = FB // NT, QB // NT, HL // NT
        d = HL * nh
        any_ = pl.BlockSpec(memory_space=pl.ANY)
        vm = pl.BlockSpec(memory_space=pltpu.VMEM)
        dma = pltpu.SemaphoreType.DMA
        V = pltpu.VMEM
        scratch = [
            V((S, HL), BF16), V((1, 2 * HL), F32), V((1, HL), F32), V((S, OL), BF16),
            V((DT, FL, NT), BF16), V((DT, OL, NT), BF16), V((2, QT, 2 * HL, NT), BF16),
            V((NB, 2, 2 * HL, NT), BF16), V((S, 2 * HL), BF16), V((C, nh, 1, 128), F32),
            V((2, TP, T, 2 * NT), F32), V((3, TP, T, 2 * NT), F32), V((2, TP, T, 2 * NT), F32),
            V((3, nh, T, FB), BF16), V((2, T, HL), F32), V((3, T, HL), F32),
            V((C, nh, 1, 128), F32), V((S, 2 * HL), BF16),
            V((C, T, QB), F32), V((C, T, QB), F32), V((C, T, QB), F32),
            dma((4,)), dma((NB,)), dma, dma, dma, dma,
            dma((2,)), dma((3,)), dma((3,)), dma((3, 3)), dma((2,)), dma((3,)), dma, dma((4,)), dma, dma, dma,
            dma((max(2 * TP, 2 * C),)), dma((C + 3,)),
        ]
        xo, qo, _ = pl.pallas_call(
            functools.partial(_kernel, T, C, float(d)),
            out_shape=(V((S, HL), BF16), V((S, QL), BF16), jax.ShapeDtypeStruct((2 * TP, 2, HL, NT), BF16)),
            in_specs=[any_] * 9,
            out_specs=(vm, vm, any_),
            scratch_shapes=scratch,
            compiler_params=pltpu.CompilerParams(collective_id=0, has_side_effects=True, vmem_limit_bytes=56 * 2**20),
            name='block',
        )(x, g1.reshape(1, HL), g2.reshape(1, HL), w_gate, w_up, w_down, o, w_o, w_qkv)
        return pl.pallas_call(
            _out_kernel,
            out_shape=(jax.ShapeDtypeStruct((S, HL), BF16), jax.ShapeDtypeStruct((S, QL), BF16)),
            in_specs=[vm, vm],
            out_specs=(any_, any_),
            scratch_shapes=[dma((2, 4))],
            compiler_params=pltpu.CompilerParams(vmem_limit_bytes=2**20),
            name='out',
        )(xo, qo)

    in_specs = (P(None, 'h'), P('h'), P('h'), P('h', 'f'), P('h', 'f'), P('f', 'h'),
                P(None, 'f'), P('f', 'h'), P('h', 'f'))
    return jax.shard_map(body, mesh=mesh, in_specs=in_specs,
                         out_specs=(P(None, 'h'), P(None, 'f')), check_vma=False)
```

```python
import functools

import jax
import jax.numpy as jnp
from jax import lax
from jax.experimental import pallas as pl
from jax.experimental.pallas import tpu as pltpu
from jax.sharding import PartitionSpec as P

EPS = 1e-6
MESH = pl.DeviceIdType.MESH
F32 = jnp.float32
BF16 = jnp.bfloat16
NT = 256
NB = 4
HOLD = 2
DIRECT = 16


def _dot(a, b):
    return jnp.dot(a, b, preferred_element_type=F32)


def _kernel(T, C, d,
            x_hbm, g1_hbm, g2_hbm, wg_hbm, wu_hbm, wd_hbm, o_hbm, wo_hbm, wq_hbm,
            xov, qall, wsib_hbm,
            xv, g1v, g2v, ov, wd, wo, wq, wbuf, nf, ss1, psnd, prcv, pkeep, abuf, ysnd, yrcv, ss2, nf2,
            qsnd, qrcv, qkeep,
            in_sem, ld_sem, w0_s, ws_s, wq_s, ss1_s, p_s, p_r, a_s, a_r, y_s, y_r, ss2_s, ss2_r, n2_s, q_s, qa_s,
            pool_a, pool_b):
    ws_r, n2_r, q_r = pool_a, pool_a.at[pl.ds(0, C)], pool_a.at[pl.ds(C, C)]
    n_s, n_r, w0_r, ss1_r, wq_r = (pool_b.at[pl.ds(0, 3)], pool_b.at[pl.ds(3, 3)], pool_b.at[pl.ds(6, 2)],
                                   pool_b.at[pl.ds(8, 2)], pool_b.at[10])
    qa_r = pool_b
    S = xv.shape[0]
    HL = xv.shape[1]
    FB = abuf.shape[3]
    QB = qsnd.shape[2]
    TP = FB // NT
    QT = QB // NT
    DT = HL // NT
    f = lax.axis_index('f')
    h = lax.axis_index('h')
    c = lax.rem(h, 2)
    xx = h // 2
    hx = (1 - xx) * 2 + c
    hs = xx * 2 + (1 - c)
    hd = (1 - xx) * 2 + (1 - c)
    XP, SIB, DIAG, YP = (f, hx), (f, hs), (f, hd), (1 - f, h)

    def rcopy(src, dst, s, r, dev):
        return pltpu.make_async_remote_copy(src_ref=src, dst_ref=dst, send_sem=s, recv_sem=r, device_id=dev,
                                            device_id_type=MESH)

    def lcopy(src, dst, s):
        return pltpu.make_async_copy(src, dst, s)

    def lwait(ref, sem):
        lcopy(ref, ref, sem).wait()

    def rwait(ref, sem):
        rcopy(ref, ref, sem, sem, XP).wait_recv()

    def mo(v, m):
        return pl.multiple_of(v, m)

    top, rest = pl.ds(0, T), pl.ds(T, S - T)
    first = [lcopy(x_hbm.at[top], xv.at[top], in_sem.at[0]), lcopy(g1_hbm, g1v.at[:, pl.ds(0, HL)], in_sem.at[1])]
    second = [lcopy(x_hbm.at[rest], xv.at[rest], in_sem.at[2]), lcopy(g2_hbm, g2v, in_sem.at[3])]
    for cp in first:
        cp.start()

    bar = pltpu.get_barrier_semaphore()
    for dev in (XP, SIB, DIAG, YP):
        pl.semaphore_signal(bar, inc=1, device_id=dev, device_id_type=MESH)

    NL = 3 * TP + (C - 2) * 2 * TP

    def tile_of(g):
        return jnp.where(g < TP, g, lax.rem(g + TP, 2 * TP))

    def own(g):
        t = tile_of(g)
        bs = lax.rem(g, NB)
        blk = jnp.where(t < TP, hx, h)
        col = mo(blk * FB + lax.rem(t, TP) * NT, NT)
        return (lcopy(wg_hbm.at[:, pl.ds(col, NT)], wbuf.at[bs, 0, pl.ds(0, HL)], ld_sem.at[bs]),
                lcopy(wu_hbm.at[:, pl.ds(col, NT)], wbuf.at[bs, 1, pl.ds(0, HL)], ld_sem.at[bs]))

    def sib(g):
        t = tile_of(g)
        bs = lax.rem(g, NB)
        return (lcopy(wsib_hbm.at[t, 0], wbuf.at[bs, 0, pl.ds(HL, HL)], ld_sem.at[bs]),
                lcopy(wsib_hbm.at[t, 1], wbuf.at[bs, 1, pl.ds(HL, HL)], ld_sem.at[bs]))

    def wcopy(t, m):
        blk = jnp.where(t < TP, hd, hs)
        col = mo(blk * FB + lax.rem(t, TP) * NT, NT)
        src = (wg_hbm, wu_hbm)[m].at[:, pl.ds(col, NT)]
        return rcopy(src, wsib_hbm.at[t, m], ws_s, ws_r.at[t], SIB)

    def wqcopy(b, t):
        blk = (hd, hs)[b]
        col = mo(blk * QB + t * NT, NT)
        return rcopy(wq_hbm.at[:, pl.ds(col, NT)], wq.at[b, t, pl.ds(HL, HL)], wq_s, wq_r, SIB)

    def start_sib(g):
        @pl.when((g <= TP) | ((g >= 2 * TP) & (g < 3 * TP)))
        def _():
            t = tile_of(g)
            rwait(wsib_hbm.at[t], ws_r.at[t])

        for cp in sib(g):
            cp.start()

    def start_own(g):
        for cp in own(g):
            cp.start()

    def wait_tile(g):
        bs = lax.rem(g, NB)
        lwait(wbuf.at[bs], ld_sem.at[bs])

    first[0].wait()
    start_own(jnp.int32(0))
    for cp in second:
        cp.start()
    start_own(jnp.int32(1))

    def row_sums(xf):
        s = jnp.broadcast_to(jnp.sum(xf * xf, axis=1, keepdims=True), (T, 128))
        if T < 128:
            s = jnp.concatenate([s] * (128 // T), axis=0)
        return s.T[0:1]

    def row_scales(ss):
        r = lax.rsqrt((ss[0] + ss[1] + ss[2] + ss[3]) / d + EPS)
        return jnp.broadcast_to(r, (128, 128)).T[0:T]

    def sums1(j):
        ss1[j, h] = row_sums(xv[pl.ds(j * T, T), :].astype(F32))

    sums1(0)

    def ss1copy(j, k):
        dev = (XP, SIB, DIAG)[k]
        return rcopy(ss1.at[j, h], ss1.at[j, h], ss1_s, ss1_r.at[min(j, 1)], dev)

    def xcopy(k):
        rows = (top, rest)[k]
        return rcopy(xv.at[rows], nf2.at[rows, pl.ds(HL, HL)], n_s.at[k], n_r.at[k], SIB)

    gcp = rcopy(g1v.at[:, pl.ds(0, HL)], g1v.at[:, pl.ds(HL, HL)], n_s.at[2], n_r.at[2], SIB)

    first[1].wait()
    pl.semaphore_wait(bar, 4)
    for k in (0, 2, 1):
        ss1copy(0, k).start()
    xcopy(0).start()
    gcp.start()
    def w0copy(m):
        src = (wg_hbm, wu_hbm)[m].at[:, pl.ds(mo(hd * FB, NT), NT)]
        return rcopy(src, wbuf.at[0, m, pl.ds(HL, HL)], w0_s, w0_r.at[m], SIB)

    for m in range(2):
        w0copy(m).start()

    @pl.loop(1, TP)
    def _(t):
        for m in range(2):
            wcopy(t, m).start()

    for m in range(2):
        wcopy(jnp.int32(0), m).start()
    for cp in second:
        cp.wait()
    for j in range(1, C):
        sums1(j)
        for k in range(3):
            ss1copy(j, k).start()
    xcopy(1).start()

    @pl.loop(TP, 2 * TP)
    def _(t):
        for m in range(2):
            wcopy(t, m).start()

    for b in range(2):
        for t in range(QT):
            wqcopy(b, t).start()

    def norm1(j):
        if j == 0:
            rwait(ss1.at[0, pl.ds(0, 3)], ss1_r.at[0])
        elif j == 1:
            rwait(ss1.at[pl.ds(1, C - 1), pl.ds(0, 3)], ss1_r.at[1])
        rr = row_scales(ss1.at[j])
        rows = pl.ds(j * T, T)
        for half in range(2):
            for l in range(HL // 128):
                cols = pl.ds(half * HL + l * 128, 128)
                xb = xv[rows, pl.ds(l * 128, 128)] if half == 0 else nf2[rows, cols]
                nf[rows, cols] = (xb.astype(F32) * rr * g1v[:, cols]).astype(BF16)

    gcp.wait_recv()
    xcopy(0).wait_recv()
    norm1(0)

    def pcopy(j, t):
        s2 = lax.rem(j, 2)
        s3 = lax.rem(j, 3)
        return rcopy(psnd.at[s2, t], prcv.at[s3, t], p_s.at[s2], p_r.at[s3], XP)

    def gu(g, row, n):
        bs = lax.rem(g, NB)
        nn = nf[pl.ds(row, n), :]
        return _dot(nn, wbuf[bs, 0]), _dot(nn, wbuf[bs, 1])

    def prefetch(g):
        @pl.when(g < NL)
        def _():
            start_own(g)
            start_sib(g)

    def put_send(j, t, gg, uu):
        s2 = lax.rem(j, 2)
        psnd[s2, t, :, 0:NT] = gg
        psnd[s2, t, :, NT:2 * NT] = uu
        pcopy(j, t).start()

    def s12(j, between):
        s2 = lax.rem(j, 2)
        g0 = 3 * TP + (j - 2) * (2 * TP)
        rwait(psnd.at[s2], p_s.at[s2])
        row = mo(j * T, T)

        @pl.loop(0, TP)
        def _(t):
            wait_tile(g0 + t)
            prefetch(g0 + t + NB - 1)
            gg, uu = gu(g0 + t, row, T)
            put_send(j, t, gg, uu)

        @pl.loop(0, TP)
        def _(t):
            wait_tile(g0 + t + TP)
            prefetch(g0 + t + TP + NB - 1)
            gg, uu = gu(g0 + t + TP, row, T)
            pkeep[s2, t, :, 0:NT] = gg
            pkeep[s2, t, :, NT:2 * NT] = uu

            @pl.when(t < DT)
            def _():
                between(t)

    def acopy(i, k):
        sl = lax.rem(i, 3)
        b = (h, h, hx)[k]
        return rcopy(abuf.at[sl, b], abuf.at[sl, b], a_s.at[sl], a_r.at[sl, k], (XP, SIB, SIB)[k])

    def s3(i):
        s2 = lax.rem(i, 2)
        sl = lax.rem(i, 3)

        rwait(prcv.at[sl], p_r.at[sl])

        @pl.loop(0, TP)
        def _(t):
            gg = pkeep[s2, t, :, 0:NT] + prcv[sl, t, :, 0:NT]
            uu = pkeep[s2, t, :, NT:2 * NT] + prcv[sl, t, :, NT:2 * NT]
            abuf[sl, h, :, pl.ds(mo(t * NT, NT), NT)] = (gg * jax.nn.sigmoid(gg) * uu).astype(BF16)

        acopy(i, 0).start()
        acopy(i, 1).start()

    def ycopy(i, n):
        s2 = lax.rem(i, 2)
        cols = pl.ds(mo(n * NT, NT), NT)
        sl = lax.rem(i, 3)
        return rcopy(ysnd.at[s2, :, cols], yrcv.at[sl, :, cols], y_s.at[s2], y_r.at[sl], YP)

    def down(sl, b, n):
        return _dot(abuf[sl, b], wd[n, pl.ds(mo(b * FB, FB), FB)])

    def down_own(i, n):
        s2 = lax.rem(i, 2)
        sl = lax.rem(i, 3)
        acc = _dot(ov[pl.ds(mo(i * T, T), T), :], wo[n])
        acc += down(sl, h, n)
        acc += down(sl, hs, n)
        ysnd[s2, :, pl.ds(mo(n * NT, NT), NT)] = acc

    def s4a(i):
        acopy(i, 1).wait_recv()

        @pl.loop(0, DT)
        def _(n):
            down_own(i, n)

    def s4b(i):
        s2 = lax.rem(i, 2)
        sl = lax.rem(i, 3)
        acopy(i, 0).wait_recv()
        acopy(i, 2).start()
        acopy(i, 2).wait_recv()

        @pl.loop(0, DT)
        def _(n):
            ysnd[s2, :, pl.ds(mo(n * NT, NT), NT)] += down(sl, hx, n) + down(sl, hd, n)
            ycopy(i, n).start()

    def ss2copy(i, k):
        dev = (XP, SIB, DIAG)[k]
        return rcopy(ss2.at[i, h], ss2.at[i, h], ss2_s, ss2_r.at[lax.rem(i, 4)], dev)

    def s5(i):
        s2 = lax.rem(i, 2)
        sl = lax.rem(i, 3)
        rwait(abuf.at[sl, pl.ds(0, 3)], a_s.at[sl])
        rwait(ysnd.at[s2], y_s.at[s2])
        rwait(yrcv.at[sl], y_r.at[sl])
        rows = pl.ds(mo(i * T, T), T)
        xn = (xv[rows, :].astype(F32) + (ysnd[s2] + yrcv[sl])).astype(BF16)
        xov[rows, :] = xn
        ss2[i, h] = row_sums(xn.astype(F32))
        for k in range(3):
            ss2copy(i, k).start()

    def n2copy(i):
        rows = pl.ds(mo(i * T, T), T)
        return rcopy(nf2.at[rows, pl.ds(0, HL)], nf2.at[rows, pl.ds(HL, HL)], n2_s, n2_r.at[i], SIB)

    def s6(i):
        rows = pl.ds(mo(i * T, T), T)
        rwait(ss2.at[i, pl.ds(0, 3)], ss2_r.at[lax.rem(i, 4)])
        rr = row_scales(ss2.at[i])
        for l in range(HL // 128):
            xf = xov[rows, pl.ds(l * 128, 128)].astype(F32)
            nf2[rows, pl.ds(l * 128, 128)] = (xf * rr * g2v[:, pl.ds(l * 128, 128)]).astype(BF16)
        n2copy(i).start()

    def qcopy(i):
        return rcopy(qsnd.at[i], qrcv.at[i], q_s, q_r.at[i], XP)

    def s7(i):
        n2copy(i).wait_recv()
        nn = nf2[pl.ds(mo(i * T, T), T), :]
        for t in range(QT):
            qsnd[i, :, t * NT:(t + 1) * NT] = _dot(nn, wq[0, t])
        qcopy(i).start()
        for t in range(QT):
            qkeep[i, :, t * NT:(t + 1) * NT] = _dot(nn, wq[1, t])

    def qacopy(i, k, last=False):
        b = (h, h, hx)[k]
        dev = (XP, SIB, SIB)[k]
        n = T - DIRECT if last and k != 1 else T
        blk = qall.at[pl.ds(mo(i * T, T), n), pl.ds(mo(b * QB, NT), QB)]
        return rcopy(blk, blk, qa_s, qa_r.at[(i, C, C + 2)[k]], dev)

    def direct(k):
        blk = qall.at[pl.ds(S - DIRECT, DIRECT), pl.ds(mo(h * QB, NT), QB)]
        return rcopy(blk, blk, qa_s, qa_r.at[C + 1], (XP, DIAG)[k])

    def s8(i, late=False):
        qcopy(i).wait_recv()
        for t in range(QT):
            cols = pl.ds(t * NT, NT)
            qall[pl.ds(mo(i * T, T), T), pl.ds(mo(h * QB + t * NT, NT), NT)] = (qkeep[i, :, cols] + qrcv[i, :, cols]).astype(BF16)
        qacopy(i, 1).start()
        if late:
            pl.when(c == 0)(qacopy(i, 0).start)
        else:
            qacopy(i, 0).start()

    def s9a(i):
        qacopy(i, 0).wait_recv()
        qacopy(i, 2).start()

    lwait(wbuf.at[0, :, pl.ds(0, HL)], ld_sem.at[0])
    for m in range(2):
        cols = pl.ds(m * NT, NT)
        rwait(wbuf.at[0, m, pl.ds(HL, HL)], w0_r.at[m])
        psnd[0, 0, :, cols] = _dot(nf[top, :], wbuf[0, m])
        rcopy(psnd.at[0, 0, :, cols], prcv.at[0, 0, :, cols], p_s.at[0], p_r.at[0], XP).start()
    start_own(jnp.int32(2))
    start_sib(jnp.int32(1))

    @pl.loop(1, TP)
    def _(t):
        wait_tile(t)
        gg, uu = gu(t, 0, T)
        put_send(jnp.int32(0), t, gg, uu)
        start_own(t + 2)
        start_sib(t + 1)

    start_sib(jnp.int32(TP + 1))
    for g in range(TP + 2, TP + NB - 1):
        prefetch(jnp.int32(g))
    xcopy(1).wait_recv()
    for j in range(1, C):
        norm1(j)

    @pl.loop(0, TP)
    def _(t):
        wait_tile(TP + t)
        prefetch(TP + t + NB - 1)
        gg, uu = gu(TP + t, T, T)
        put_send(jnp.int32(1), t, gg, uu)


    res = [[] for _ in range(4)]
    for n in range(DT):
        res[n % 4].append(lcopy(wd_hbm.at[:, pl.ds(n * NT, NT)], wd.at[n], in_sem.at[1]))
        res[n % 4].append(lcopy(wo_hbm.at[:, pl.ds(n * NT, NT)], wo.at[n], in_sem.at[2]))
    res[0].append(lcopy(o_hbm, ov, in_sem.at[0]))
    for b in range(2):
        blk = (hx, h)[b]
        for t in range(QT):
            res[3].append(lcopy(wq_hbm.at[:, pl.ds(mo(blk * QB + t * NT, NT), NT)], wq.at[b, t, pl.ds(0, HL)],
                                in_sem.at[3]))

    @pl.loop(0, TP)
    def _(t):
        wait_tile(2 * TP + t)
        prefetch(2 * TP + t + NB - 1)
        for k in range(4):
            @pl.when(t == k)
            def _(k=k):
                for cp in res[k]:
                    cp.start()

        gg, uu = gu(2 * TP + t, 0, 2 * T)
        for j in range(2):
            pkeep[j, t, :, 0:NT] = gg[j * T:(j + 1) * T]
            pkeep[j, t, :, NT:2 * NT] = uu[j * T:(j + 1) * T]

    gcp.wait_send()
    rwait(ss1.at[:, pl.ds(0, 3)], ss1_s)
    for k in range(2):
        xcopy(k).wait_send()

    def stage(fn, i, lo=0):
        @pl.when((i >= lo) & (i < C))
        def _():
            fn(i)

    def loaded():
        lwait(ov, in_sem.at[0])
        lwait(wd, in_sem.at[1])
        lwait(wo, in_sem.at[2])
        lwait(wq.at[:, :, pl.ds(0, HL)], in_sem.at[3])
        rwait(wq.at[:, :, pl.ds(HL, HL)], wq_s)
        rwait(wq.at[:, :, pl.ds(HL, HL)], wq_r)

    @pl.loop(0, C - 2)
    def _(i):
        s3(i)

        @pl.when(i == 0)
        def _():
            loaded()

        def between(n):
            @pl.when(n == 0)
            def _():
                acopy(i, 1).wait_recv()

            down_own(i, n)

        s12(i + 2, between)
        stage(s5, i - 1)
        s4b(i)
        stage(s6, i - 2)

    e = C - 1
    done = {s7: 0, s8: 0, s9a: 0}

    def run(*steps):
        for fn, i in steps:
            fn(jnp.int32(i))

    def nxt(*fns):
        for fn in fns:
            if done[fn] < C:
                fn(jnp.int32(done[fn]))
                done[fn] += 1

    run((s3, e - 1), (s4a, e - 1), (s5, e - 2), (s6, e - 3), (s3, e))
    nxt(s7)
    run((s4b, e - 1))
    nxt(s7)
    run((s4a, e), (s6, e - 2), (s4b, e))
    nxt(s7, s8)
    run((s5, e - 1))
    nxt(s7, s8)
    run((s5, e), (s6, e - 1))
    nxt(s7, s8)
    run((s6, e))
    nxt(s7, s8, s9a, s7, s8, s9a, s7, s9a)
    rwait(wsib_hbm, ws_s)
    rwait(wbuf.at[0, :, pl.ds(HL, HL)], w0_s)

    for k in range(2):
        rwait(psnd.at[k], p_s.at[k])

    while done[s8] < C - HOLD - 1:
        nxt(s8, s9a)
    while done[s8] < C - 1:
        s8(jnp.int32(done[s8]), late=True)
        done[s8] += 1
        if done[s9a] < C - HOLD - 1:
            nxt(s9a)

    s8(jnp.int32(C - 1), late=True)

    @pl.when(c == 1)
    def _():
        for i in range(C - HOLD - 1, C - 1):
            qacopy(jnp.int32(i), 0).start()
        qacopy(jnp.int32(C - 1), 0, last=True).start()
        direct(0).start()
        direct(1).start()

    rwait(ss2.at[:, pl.ds(0, 3)], ss2_s)
    rwait(nf2.at[:, pl.ds(0, HL)], n2_s)
    rwait(qsnd, q_s)

    while done[s9a] < C - 1:
        nxt(s9a)
    e = jnp.int32(C - 1)
    rows = pl.ds(0, DIRECT)

    @pl.when(c == 0)
    def _():
        s9a(e)
        rwait(qall.at[pl.ds(0, S - DIRECT), pl.ds(0, QB)], qa_r.at[C + 2])
        rwait(qall.at[rows, pl.ds(0, QB)], qa_r.at[C + 1])

    @pl.when(c == 1)
    def _():
        qacopy(e, 0, last=True).wait_recv()
        qacopy(e, 2, last=True).start()
        rwait(qall.at[:, pl.ds(0, QB)], qa_r.at[C + 2])
        rwait(qall.at[rows, pl.ds(0, QB)], qa_r.at[C + 1])

    rwait(qall.at[:, pl.ds(0, QB)], qa_r.at[C])
    rwait(qall.at[:, pl.ds(0, 3 * QB)], qa_s)


def _out_kernel(xv, qv, xo, qo, sem):
    n = xv.shape[0] // 4
    cps = [pltpu.make_async_copy(a.at[pl.ds(k * n, n)], b.at[pl.ds(k * n, n)], sem.at[m])
           for m, (a, b) in enumerate(((qv, qo), (xv, xo))) for k in range(4)]
    for cp in cps:
        cp.start()
    for m, (a, b) in enumerate(((qv, qo), (xv, xo))):
        pltpu.make_async_copy(a, b, sem.at[m]).wait()


def solution(mesh):
    nh = mesh.shape['h']

    def body(x, g1, g2, w_gate, w_up, w_down, o, w_o, w_qkv):
        S, HL = x.shape
        FL = w_gate.shape[1]
        FB = FL // nh
        QL = w_qkv.shape[1]
        QB = QL // nh
        OL = o.shape[1]
        T = 64
        C = S // T
        TP, QT, DT = FB // NT, QB // NT, HL // NT
        d = HL * nh
        any_ = pl.BlockSpec(memory_space=pl.ANY)
        vm = pl.BlockSpec(memory_space=pltpu.VMEM)
        dma = pltpu.SemaphoreType.DMA
        V = pltpu.VMEM
        scratch = [
            V((S, HL), BF16), V((1, 2 * HL), F32), V((1, HL), F32), V((S, OL), BF16),
            V((DT, FL, NT), BF16), V((DT, OL, NT), BF16), V((2, QT, 2 * HL, NT), BF16),
            V((NB, 2, 2 * HL, NT), BF16), V((S, 2 * HL), BF16), V((C, nh, 1, 128), F32),
            V((2, TP, T, 2 * NT), F32), V((3, TP, T, 2 * NT), F32), V((2, TP, T, 2 * NT), F32),
            V((3, nh, T, FB), BF16), V((2, T, HL), F32), V((3, T, HL), F32),
            V((C, nh, 1, 128), F32), V((S, 2 * HL), BF16),
            V((C, T, QB), F32), V((C, T, QB), F32), V((C, T, QB), F32),
            dma((4,)), dma((NB,)), dma, dma, dma, dma,
            dma((2,)), dma((3,)), dma((3,)), dma((3, 3)), dma((2,)), dma((3,)), dma, dma((4,)), dma, dma, dma,
            dma((max(2 * TP, 2 * C),)), dma((C + 3,)),
        ]
        xo, qo, _ = pl.pallas_call(
            functools.partial(_kernel, T, C, float(d)),
            out_shape=(V((S, HL), BF16), V((S, QL), BF16), jax.ShapeDtypeStruct((2 * TP, 2, HL, NT), BF16)),
            in_specs=[any_] * 9,
            out_specs=(vm, vm, any_),
            scratch_shapes=scratch,
            compiler_params=pltpu.CompilerParams(collective_id=0, has_side_effects=True, vmem_limit_bytes=56 * 2**20),
            name='block',
        )(x, g1.reshape(1, HL), g2.reshape(1, HL), w_gate, w_up, w_down, o, w_o, w_qkv)
        return pl.pallas_call(
            _out_kernel,
            out_shape=(jax.ShapeDtypeStruct((S, HL), BF16), jax.ShapeDtypeStruct((S, QL), BF16)),
            in_specs=[vm, vm],
            out_specs=(any_, any_),
            scratch_shapes=[dma((2,))],
            compiler_params=pltpu.CompilerParams(vmem_limit_bytes=2**20),
            name='out',
        )(xo, qo)

    in_specs = (P(None, 'h'), P('h'), P('h'), P('h', 'f'), P('h', 'f'), P('f', 'h'),
                P(None, 'f'), P('f', 'h'), P('h', 'f'))
    return jax.shard_map(body, mesh=mesh, in_specs=in_specs,
                         out_specs=(P(None, 'h'), P(None, 'f')), check_vma=False)
```

```python
import functools

import jax
import jax.numpy as jnp
from jax import lax
from jax.experimental import pallas as pl
from jax.experimental.pallas import tpu as pltpu
from jax.sharding import PartitionSpec as P

EPS = 1e-6
MESH = pl.DeviceIdType.MESH
F32 = jnp.float32
BF16 = jnp.bfloat16
NT = 256
NB = 4
HOLD = 2
DIRECT = 16


def _dot(a, b):
    return jnp.dot(a, b, preferred_element_type=F32)


def _kernel(T, C, d,
            x_hbm, g1_hbm, g2_hbm, wg_hbm, wu_hbm, wd_hbm, o_hbm, wo_hbm, wq_hbm,
            xov, qall, wsib_hbm,
            xv, g1v, g2v, ov, wd, wo, wq, wbuf, nf, ss1, psnd, prcv, pkeep, abuf, ysnd, yrcv, ss2, nf2,
            qsnd, qrcv, qkeep,
            in_sem, ld_sem, w0_s, ws_s, wq_s, ss1_s, p_s, p_r, a_s, a_r, y_s, y_r, ss2_r,
            pool_a, pool_b):
    ws_r, n2_r, q_r = pool_a, pool_a.at[pl.ds(0, C)], pool_a.at[pl.ds(C, C)]
    n_s, n_r, w0_r, ss1_r, wq_r = (pool_b.at[pl.ds(0, 3)], pool_b.at[pl.ds(3, 3)], pool_b.at[pl.ds(6, 2)],
                                   pool_b.at[pl.ds(8, 2)], pool_b.at[10])
    qa_r = pool_b
    ss2_s, n2_s, q_s, qa_s = ss1_s, ws_s, wq_s, w0_s
    S = xv.shape[0]
    HL = xv.shape[1]
    FB = abuf.shape[3]
    QB = qsnd.shape[2]
    TP = FB // NT
    QT = QB // NT
    DT = HL // NT
    f = lax.axis_index('f')
    h = lax.axis_index('h')
    c = lax.rem(h, 2)
    xx = h // 2
    hx = (1 - xx) * 2 + c
    hs = xx * 2 + (1 - c)
    hd = (1 - xx) * 2 + (1 - c)
    XP, SIB, DIAG, YP = (f, hx), (f, hs), (f, hd), (1 - f, h)

    def rcopy(src, dst, s, r, dev):
        return pltpu.make_async_remote_copy(src_ref=src, dst_ref=dst, send_sem=s, recv_sem=r, device_id=dev,
                                            device_id_type=MESH)

    def lcopy(src, dst, s):
        return pltpu.make_async_copy(src, dst, s)

    def lwait(ref, sem):
        lcopy(ref, ref, sem).wait()

    def rwait(ref, sem):
        rcopy(ref, ref, sem, sem, XP).wait_recv()

    def mo(v, m):
        return pl.multiple_of(v, m)

    top, rest = pl.ds(0, T), pl.ds(T, S - T)
    first = [lcopy(x_hbm.at[top], xv.at[top], in_sem.at[0]), lcopy(g1_hbm, g1v.at[:, pl.ds(0, HL)], in_sem.at[1])]
    second = [lcopy(x_hbm.at[rest], xv.at[rest], in_sem.at[2]), lcopy(g2_hbm, g2v, in_sem.at[3])]
    for cp in first:
        cp.start()

    bar = pltpu.get_barrier_semaphore()
    for dev in (XP, SIB, DIAG, YP):
        pl.semaphore_signal(bar, inc=1, device_id=dev, device_id_type=MESH)

    NL = 3 * TP + (C - 2) * 2 * TP

    def tile_of(g):
        return jnp.where(g < TP, g, lax.rem(g + TP, 2 * TP))

    def own(g):
        t = tile_of(g)
        bs = lax.rem(g, NB)
        blk = jnp.where(t < TP, hx, h)
        col = mo(blk * FB + lax.rem(t, TP) * NT, NT)
        return (lcopy(wg_hbm.at[:, pl.ds(col, NT)], wbuf.at[bs, 0, pl.ds(0, HL)], ld_sem.at[bs]),
                lcopy(wu_hbm.at[:, pl.ds(col, NT)], wbuf.at[bs, 1, pl.ds(0, HL)], ld_sem.at[bs]))

    def sib(g):
        t = tile_of(g)
        bs = lax.rem(g, NB)
        return (lcopy(wsib_hbm.at[t, 0], wbuf.at[bs, 0, pl.ds(HL, HL)], ld_sem.at[bs]),
                lcopy(wsib_hbm.at[t, 1], wbuf.at[bs, 1, pl.ds(HL, HL)], ld_sem.at[bs]))

    def wcopy(t, m):
        blk = jnp.where(t < TP, hd, hs)
        col = mo(blk * FB + lax.rem(t, TP) * NT, NT)
        src = (wg_hbm, wu_hbm)[m].at[:, pl.ds(col, NT)]
        return rcopy(src, wsib_hbm.at[t, m], ws_s, ws_r.at[t], SIB)

    def wqcopy(b, t):
        blk = (hd, hs)[b]
        col = mo(blk * QB + t * NT, NT)
        return rcopy(wq_hbm.at[:, pl.ds(col, NT)], wq.at[b, t, pl.ds(HL, HL)], wq_s, wq_r, SIB)

    def start_sib(g):
        @pl.when((g <= TP) | ((g >= 2 * TP) & (g < 3 * TP)))
        def _():
            t = tile_of(g)
            rwait(wsib_hbm.at[t], ws_r.at[t])

        for cp in sib(g):
            cp.start()

    def start_own(g):
        for cp in own(g):
            cp.start()

    def wait_tile(g):
        bs = lax.rem(g, NB)
        lwait(wbuf.at[bs], ld_sem.at[bs])

    first[0].wait()
    start_own(jnp.int32(0))
    for cp in second:
        cp.start()
    start_own(jnp.int32(1))

    def row_sums(xf):
        s = jnp.broadcast_to(jnp.sum(xf * xf, axis=1, keepdims=True), (T, 128))
        if T < 128:
            s = jnp.concatenate([s] * (128 // T), axis=0)
        return s.T[0:1]

    def row_scales(ss):
        r = lax.rsqrt((ss[0] + ss[1] + ss[2] + ss[3]) / d + EPS)
        return jnp.broadcast_to(r, (128, 128)).T[0:T]

    def sums1(j):
        ss1[j, h] = row_sums(xv[pl.ds(j * T, T), :].astype(F32))

    sums1(0)

    def ss1copy(j, k):
        dev = (XP, SIB, DIAG)[k]
        return rcopy(ss1.at[j, h], ss1.at[j, h], ss1_s, ss1_r.at[min(j, 1)], dev)

    def xcopy(k):
        rows = (top, rest)[k]
        return rcopy(xv.at[rows], nf2.at[rows, pl.ds(HL, HL)], n_s.at[k], n_r.at[k], SIB)

    gcp = rcopy(g1v.at[:, pl.ds(0, HL)], g1v.at[:, pl.ds(HL, HL)], n_s.at[2], n_r.at[2], SIB)

    first[1].wait()
    pl.semaphore_wait(bar, 4)
    for k in (0, 2, 1):
        ss1copy(0, k).start()
    xcopy(0).start()
    gcp.start()
    def w0copy(m):
        src = (wg_hbm, wu_hbm)[m].at[:, pl.ds(mo(hd * FB, NT), NT)]
        return rcopy(src, wbuf.at[0, m, pl.ds(HL, HL)], w0_s, w0_r.at[m], SIB)

    for m in range(2):
        w0copy(m).start()

    @pl.loop(1, TP)
    def _(t):
        for m in range(2):
            wcopy(t, m).start()

    for m in range(2):
        wcopy(jnp.int32(0), m).start()
    for cp in second:
        cp.wait()
    for j in range(1, C):
        sums1(j)
        for k in range(3):
            ss1copy(j, k).start()
    xcopy(1).start()

    @pl.loop(TP, 2 * TP)
    def _(t):
        for m in range(2):
            wcopy(t, m).start()

    for b in range(2):
        for t in range(QT):
            wqcopy(b, t).start()

    def norm1(j):
        if j == 0:
            rwait(ss1.at[0, pl.ds(0, 3)], ss1_r.at[0])
        elif j == 1:
            rwait(ss1.at[pl.ds(1, C - 1), pl.ds(0, 3)], ss1_r.at[1])
        rr = row_scales(ss1.at[j])
        rows = pl.ds(j * T, T)
        for half in range(2):
            for l in range(HL // 128):
                cols = pl.ds(half * HL + l * 128, 128)
                xb = xv[rows, pl.ds(l * 128, 128)] if half == 0 else nf2[rows, cols]
                nf[rows, cols] = (xb.astype(F32) * rr * g1v[:, cols]).astype(BF16)

    gcp.wait_recv()
    xcopy(0).wait_recv()
    norm1(0)

    def pcopy(j, t):
        s2 = lax.rem(j, 2)
        s3 = lax.rem(j, 3)
        return rcopy(psnd.at[s2, t], prcv.at[s3, t], p_s.at[s2], p_r.at[s3], XP)

    def gu(g, row, n):
        bs = lax.rem(g, NB)
        nn = nf[pl.ds(row, n), :]
        return _dot(nn, wbuf[bs, 0]), _dot(nn, wbuf[bs, 1])

    def prefetch(g):
        @pl.when(g < NL)
        def _():
            start_own(g)
            start_sib(g)

    def put_send(j, t, gg, uu):
        s2 = lax.rem(j, 2)
        psnd[s2, t, :, 0:NT] = gg
        psnd[s2, t, :, NT:2 * NT] = uu
        pcopy(j, t).start()

    def s12(j, between):
        s2 = lax.rem(j, 2)
        g0 = 3 * TP + (j - 2) * (2 * TP)
        rwait(psnd.at[s2], p_s.at[s2])
        row = mo(j * T, T)

        @pl.loop(0, TP)
        def _(t):
            wait_tile(g0 + t)
            prefetch(g0 + t + NB - 1)
            gg, uu = gu(g0 + t, row, T)
            put_send(j, t, gg, uu)

        @pl.loop(0, TP)
        def _(t):
            wait_tile(g0 + t + TP)
            prefetch(g0 + t + TP + NB - 1)
            gg, uu = gu(g0 + t + TP, row, T)
            pkeep[s2, t, :, 0:NT] = gg
            pkeep[s2, t, :, NT:2 * NT] = uu

            @pl.when(t < DT)
            def _():
                between(t)

    def acopy(i, k):
        sl = lax.rem(i, 3)
        b = (h, h, hx)[k]
        return rcopy(abuf.at[sl, b], abuf.at[sl, b], a_s.at[sl], a_r.at[sl, k], (XP, SIB, SIB)[k])

    def s3(i):
        s2 = lax.rem(i, 2)
        sl = lax.rem(i, 3)

        rwait(prcv.at[sl], p_r.at[sl])

        @pl.loop(0, TP)
        def _(t):
            gg = pkeep[s2, t, :, 0:NT] + prcv[sl, t, :, 0:NT]
            uu = pkeep[s2, t, :, NT:2 * NT] + prcv[sl, t, :, NT:2 * NT]
            abuf[sl, h, :, pl.ds(mo(t * NT, NT), NT)] = (gg * jax.nn.sigmoid(gg) * uu).astype(BF16)

        acopy(i, 0).start()
        acopy(i, 1).start()

    def ycopy(i, n):
        s2 = lax.rem(i, 2)
        cols = pl.ds(mo(n * NT, NT), NT)
        sl = lax.rem(i, 3)
        return rcopy(ysnd.at[s2, :, cols], yrcv.at[sl, :, cols], y_s.at[s2], y_r.at[sl], YP)

    def down(sl, b, n):
        return _dot(abuf[sl, b], wd[n, pl.ds(mo(b * FB, FB), FB)])

    def down_own(i, n):
        s2 = lax.rem(i, 2)
        sl = lax.rem(i, 3)
        acc = _dot(ov[pl.ds(mo(i * T, T), T), :], wo[n])
        acc += down(sl, h, n)
        acc += down(sl, hs, n)
        ysnd[s2, :, pl.ds(mo(n * NT, NT), NT)] = acc

    def s4a(i):
        acopy(i, 1).wait_recv()

        @pl.loop(0, DT)
        def _(n):
            down_own(i, n)

    def s4b(i):
        s2 = lax.rem(i, 2)
        sl = lax.rem(i, 3)
        acopy(i, 0).wait_recv()
        acopy(i, 2).start()
        acopy(i, 2).wait_recv()

        @pl.loop(0, DT)
        def _(n):
            ysnd[s2, :, pl.ds(mo(n * NT, NT), NT)] += down(sl, hx, n) + down(sl, hd, n)
            ycopy(i, n).start()

    def ss2copy(i, k):
        dev = (XP, SIB, DIAG)[k]
        return rcopy(ss2.at[i, h], ss2.at[i, h], ss2_s, ss2_r.at[lax.rem(i, 4)], dev)

    def s5(i):
        s2 = lax.rem(i, 2)
        sl = lax.rem(i, 3)
        rwait(abuf.at[sl, pl.ds(0, 3)], a_s.at[sl])
        rwait(ysnd.at[s2], y_s.at[s2])
        rwait(yrcv.at[sl], y_r.at[sl])
        rows = pl.ds(mo(i * T, T), T)
        xn = (xv[rows, :].astype(F32) + (ysnd[s2] + yrcv[sl])).astype(BF16)
        xov[rows, :] = xn
        ss2[i, h] = row_sums(xn.astype(F32))
        for k in range(3):
            ss2copy(i, k).start()

    def n2copy(i):
        rows = pl.ds(mo(i * T, T), T)
        return rcopy(nf2.at[rows, pl.ds(0, HL)], nf2.at[rows, pl.ds(HL, HL)], n2_s, n2_r.at[i], SIB)

    def s6(i):
        rows = pl.ds(mo(i * T, T), T)
        rwait(ss2.at[i, pl.ds(0, 3)], ss2_r.at[lax.rem(i, 4)])
        rr = row_scales(ss2.at[i])
        for l in range(HL // 128):
            xf = xov[rows, pl.ds(l * 128, 128)].astype(F32)
            nf2[rows, pl.ds(l * 128, 128)] = (xf * rr * g2v[:, pl.ds(l * 128, 128)]).astype(BF16)
        n2copy(i).start()

    def qcopy(i):
        return rcopy(qsnd.at[i], qrcv.at[i], q_s, q_r.at[i], XP)

    def s7(i):
        n2copy(i).wait_recv()
        nn = nf2[pl.ds(mo(i * T, T), T), :]
        for t in range(QT):
            qsnd[i, :, t * NT:(t + 1) * NT] = _dot(nn, wq[0, t])
        qcopy(i).start()
        for t in range(QT):
            qkeep[i, :, t * NT:(t + 1) * NT] = _dot(nn, wq[1, t])

    def qacopy(i, k, last=False):
        b = (h, h, hx)[k]
        dev = (XP, SIB, SIB)[k]
        n = T - DIRECT if last and k != 1 else T
        blk = qall.at[pl.ds(mo(i * T, T), n), pl.ds(mo(b * QB, NT), QB)]
        return rcopy(blk, blk, qa_s, qa_r.at[(i, C, C + 2)[k]], dev)

    def direct(k):
        blk = qall.at[pl.ds(S - DIRECT, DIRECT), pl.ds(mo(h * QB, NT), QB)]
        return rcopy(blk, blk, qa_s, qa_r.at[C + 1], (XP, DIAG)[k])

    def s8(i, late=False):
        qcopy(i).wait_recv()
        for t in range(QT):
            cols = pl.ds(t * NT, NT)
            qall[pl.ds(mo(i * T, T), T), pl.ds(mo(h * QB + t * NT, NT), NT)] = (qkeep[i, :, cols] + qrcv[i, :, cols]).astype(BF16)
        qacopy(i, 1).start()
        if late:
            pl.when(c == 0)(qacopy(i, 0).start)
        else:
            qacopy(i, 0).start()

    def s9a(i):
        qacopy(i, 0).wait_recv()
        qacopy(i, 2).start()

    lwait(wbuf.at[0, :, pl.ds(0, HL)], ld_sem.at[0])
    for m in range(2):
        cols = pl.ds(m * NT, NT)
        rwait(wbuf.at[0, m, pl.ds(HL, HL)], w0_r.at[m])
        psnd[0, 0, :, cols] = _dot(nf[top, :], wbuf[0, m])
        rcopy(psnd.at[0, 0, :, cols], prcv.at[0, 0, :, cols], p_s.at[0], p_r.at[0], XP).start()
    start_own(jnp.int32(2))
    start_sib(jnp.int32(1))

    @pl.loop(1, TP)
    def _(t):
        wait_tile(t)
        gg, uu = gu(t, 0, T)
        put_send(jnp.int32(0), t, gg, uu)
        start_own(t + 2)
        start_sib(t + 1)

    start_sib(jnp.int32(TP + 1))
    for g in range(TP + 2, TP + NB - 1):
        prefetch(jnp.int32(g))
    xcopy(1).wait_recv()
    for j in range(1, C):
        norm1(j)

    @pl.loop(0, TP)
    def _(t):
        wait_tile(TP + t)
        prefetch(TP + t + NB - 1)
        gg, uu = gu(TP + t, T, T)
        put_send(jnp.int32(1), t, gg, uu)


    res = [[] for _ in range(4)]
    for n in range(DT):
        res[n % 4].append(lcopy(wd_hbm.at[:, pl.ds(n * NT, NT)], wd.at[n], in_sem.at[1]))
        res[n % 4].append(lcopy(wo_hbm.at[:, pl.ds(n * NT, NT)], wo.at[n], in_sem.at[2]))
    res[0].append(lcopy(o_hbm, ov, in_sem.at[0]))
    for b in range(2):
        blk = (hx, h)[b]
        for t in range(QT):
            res[3].append(lcopy(wq_hbm.at[:, pl.ds(mo(blk * QB + t * NT, NT), NT)], wq.at[b, t, pl.ds(0, HL)],
                                in_sem.at[3]))

    @pl.loop(0, TP)
    def _(t):
        wait_tile(2 * TP + t)
        prefetch(2 * TP + t + NB - 1)
        for k in range(4):
            @pl.when(t == k)
            def _(k=k):
                for cp in res[k]:
                    cp.start()

        gg, uu = gu(2 * TP + t, 0, 2 * T)
        for j in range(2):
            pkeep[j, t, :, 0:NT] = gg[j * T:(j + 1) * T]
            pkeep[j, t, :, NT:2 * NT] = uu[j * T:(j + 1) * T]

    gcp.wait_send()
    rwait(ss1.at[:, pl.ds(0, 3)], ss1_s)
    for k in range(2):
        xcopy(k).wait_send()

    def stage(fn, i, lo=0):
        @pl.when((i >= lo) & (i < C))
        def _():
            fn(i)

    def loaded():
        lwait(ov, in_sem.at[0])
        lwait(wd, in_sem.at[1])
        lwait(wo, in_sem.at[2])
        lwait(wq.at[:, :, pl.ds(0, HL)], in_sem.at[3])
        rwait(wq.at[:, :, pl.ds(HL, HL)], wq_s)
        rwait(wq.at[:, :, pl.ds(HL, HL)], wq_r)
        rwait(wsib_hbm, ws_s)
        rwait(wbuf.at[0, :, pl.ds(HL, HL)], w0_s)

    @pl.loop(0, C - 2)
    def _(i):
        s3(i)

        @pl.when(i == 0)
        def _():
            loaded()

        def between(n):
            @pl.when(n == 0)
            def _():
                acopy(i, 1).wait_recv()

            down_own(i, n)

        s12(i + 2, between)
        stage(s5, i - 1)
        s4b(i)
        stage(s6, i - 2)

    e = C - 1
    done = {s7: 0, s8: 0, s9a: 0}

    def run(*steps):
        for fn, i in steps:
            fn(jnp.int32(i))

    def nxt(*fns):
        for fn in fns:
            if done[fn] < C:
                fn(jnp.int32(done[fn]))
                done[fn] += 1

    run((s3, e - 1), (s4a, e - 1), (s5, e - 2), (s6, e - 3), (s3, e))
    nxt(s7)
    run((s4b, e - 1))
    nxt(s7)
    run((s4a, e), (s6, e - 2), (s4b, e))
    nxt(s7, s8)
    run((s5, e - 1))
    nxt(s7, s8)
    run((s5, e), (s6, e - 1))
    nxt(s7, s8)
    run((s6, e))
    nxt(s7, s8, s9a, s7, s8, s9a, s7, s9a)

    for k in range(2):
        rwait(psnd.at[k], p_s.at[k])

    while done[s8] < C - HOLD - 1:
        nxt(s8, s9a)
    while done[s8] < C - 1:
        s8(jnp.int32(done[s8]), late=True)
        done[s8] += 1
        if done[s9a] < C - HOLD - 1:
            nxt(s9a)

    s8(jnp.int32(C - 1), late=True)

    @pl.when(c == 1)
    def _():
        for i in range(C - HOLD - 1, C - 1):
            qacopy(jnp.int32(i), 0).start()
        qacopy(jnp.int32(C - 1), 0, last=True).start()
        direct(0).start()
        direct(1).start()

    rwait(ss2.at[:, pl.ds(0, 3)], ss2_s)
    rwait(nf2.at[:, pl.ds(0, HL)], n2_s)
    rwait(qsnd, q_s)

    while done[s9a] < C - 1:
        nxt(s9a)
    e = jnp.int32(C - 1)
    rows = pl.ds(0, DIRECT)

    @pl.when(c == 0)
    def _():
        s9a(e)
        rwait(qall.at[pl.ds(0, S - DIRECT), pl.ds(0, QB)], qa_r.at[C + 2])
        rwait(qall.at[rows, pl.ds(0, QB)], qa_r.at[C + 1])

    @pl.when(c == 1)
    def _():
        qacopy(e, 0, last=True).wait_recv()
        qacopy(e, 2, last=True).start()
        rwait(qall.at[:, pl.ds(0, QB)], qa_r.at[C + 2])
        rwait(qall.at[rows, pl.ds(0, QB)], qa_r.at[C + 1])

    rwait(qall.at[:, pl.ds(0, QB)], qa_r.at[C])
    rwait(qall.at[:, pl.ds(0, 3 * QB)], qa_s)


def _out_kernel(xv, qv, xo, qo, sem):
    n = xv.shape[0] // 4
    cps = [pltpu.make_async_copy(a.at[pl.ds(k * n, n)], b.at[pl.ds(k * n, n)], sem.at[m])
           for m, (a, b) in enumerate(((qv, qo), (xv, xo))) for k in range(4)]
    for cp in cps:
        cp.start()
    for m, (a, b) in enumerate(((qv, qo), (xv, xo))):
        pltpu.make_async_copy(a, b, sem.at[m]).wait()


def solution(mesh):
    nh = mesh.shape['h']

    def body(x, g1, g2, w_gate, w_up, w_down, o, w_o, w_qkv):
        S, HL = x.shape
        FL = w_gate.shape[1]
        FB = FL // nh
        QL = w_qkv.shape[1]
        QB = QL // nh
        OL = o.shape[1]
        T = 64
        C = S // T
        TP, QT, DT = FB // NT, QB // NT, HL // NT
        d = HL * nh
        any_ = pl.BlockSpec(memory_space=pl.ANY)
        vm = pl.BlockSpec(memory_space=pltpu.VMEM)
        dma = pltpu.SemaphoreType.DMA
        V = pltpu.VMEM
        scratch = [
            V((S, HL), BF16), V((1, 2 * HL), F32), V((1, HL), F32), V((S, OL), BF16),
            V((DT, FL, NT), BF16), V((DT, OL, NT), BF16), V((2, QT, 2 * HL, NT), BF16),
            V((NB, 2, 2 * HL, NT), BF16), V((S, 2 * HL), BF16), V((C, nh, 1, 128), F32),
            V((2, TP, T, 2 * NT), F32), V((3, TP, T, 2 * NT), F32), V((2, TP, T, 2 * NT), F32),
            V((3, nh, T, FB), BF16), V((2, T, HL), F32), V((3, T, HL), F32),
            V((C, nh, 1, 128), F32), V((S, 2 * HL), BF16),
            V((C, T, QB), F32), V((C, T, QB), F32), V((C, T, QB), F32),
            dma((4,)), dma((NB,)), dma, dma, dma, dma,
            dma((2,)), dma((3,)), dma((3,)), dma((3, 3)), dma((2,)), dma((3,)), dma((4,)),
            dma((max(2 * TP, 2 * C),)), dma((C + 3,)),
        ]
        xo, qo, _ = pl.pallas_call(
            functools.partial(_kernel, T, C, float(d)),
            out_shape=(V((S, HL), BF16), V((S, QL), BF16), jax.ShapeDtypeStruct((2 * TP, 2, HL, NT), BF16)),
            in_specs=[any_] * 9,
            out_specs=(vm, vm, any_),
            scratch_shapes=scratch,
            compiler_params=pltpu.CompilerParams(collective_id=0, has_side_effects=True, vmem_limit_bytes=56 * 2**20),
            name='block',
        )(x, g1.reshape(1, HL), g2.reshape(1, HL), w_gate, w_up, w_down, o, w_o, w_qkv)
        return pl.pallas_call(
            _out_kernel,
            out_shape=(jax.ShapeDtypeStruct((S, HL), BF16), jax.ShapeDtypeStruct((S, QL), BF16)),
            in_specs=[vm, vm],
            out_specs=(any_, any_),
            scratch_shapes=[dma((2,))],
            compiler_params=pltpu.CompilerParams(vmem_limit_bytes=2**20),
            name='out',
        )(xo, qo)

    in_specs = (P(None, 'h'), P('h'), P('h'), P('h', 'f'), P('h', 'f'), P('f', 'h'),
                P(None, 'f'), P('f', 'h'), P('h', 'f'))
    return jax.shard_map(body, mesh=mesh, in_specs=in_specs,
                         out_specs=(P(None, 'h'), P(None, 'f')), check_vma=False)
```
